32 devices in a mesh: cells: 8 (over y, x, core), genes: 4 (over z).
Axes of the slice: x: 2, y: 2, z: 4, core: 2. Of those that a mesh axis runs over, the one named last changes fastest.
Arguments:
- counts: int32 [8192, 4096], P('cells', 'genes'), may hold values from 0 to 26, as said below
- library: int32 [8192], P('cells'), may hold values from 2000 to 19999
Outputs:
- adjacency: float32 [4096, 4096], P('cells', 'genes')
- connectivity: float32 [4096], P('cells')
The draws below stay inside these ranges and needn't reach their ends.
Inputs may be any that keep to these rules, and one draw needn't show every extreme that they name: Non-negative integer counts.
All inputs are finite; a program needn't handle non-finite values.
Results may differ from the reference program's by a relative error of at most 0.006.
Values may be sent and summed in bfloat16 or wider, within the bound.
A program may use at most 128 MiB of HBM per device.

```python
import jax
import jax.numpy as jnp
from jax import lax

G = 4096
CELLS_DEV = 1024
CELLS = 8192
N_CELLS = 8


module_count = 32


def draw_counts(key, part):
    module_ids = jax.random.randint(jax.random.fold_in(key, 11), (G,), 0, module_count)
    levels = jax.random.randint(jax.random.fold_in(key, 12), (CELLS, module_count), 0, 8)
    gains = jax.random.randint(jax.random.fold_in(key, 13), (G,), 0, 4)
    noise = jax.random.randint(jax.random.fold_in(key, 14), (CELLS, G), 0, 6)
    present = jax.random.randint(jax.random.fold_in(key, 15), (CELLS, G), 0, 3)
    shared = jnp.take(levels, module_ids, axis=1)
    values = noise + gains[None, :] * shared
    return jnp.where(present > 0, values, 0).astype(jnp.int32)


def place_ends(values, rng, low, high):
    longest = values.shape.index(max(values.shape))
    spots = []
    for shift in (0, 1):
        where = [jax.random.randint(jax.random.fold_in(rng, axis), (), 0, length) for axis, length in enumerate(values.shape)]
        where[longest] = (where[longest] + shift) % values.shape[longest]
        spots.append(tuple(where))
    return values.at[spots[0]].set(low).at[spots[1]].set(high)


def setup_inputs(seed: int = 0) -> dict:
    splits = jax.random.split(jax.random.key(seed), 3)
    return {
        "counts": draw_counts(jax.random.fold_in(splits[2], 71), 0),
        "library": place_ends(jax.random.randint(splits[1], (CELLS,), 2000, 20000), jax.random.fold_in(splits[1], 1), 2000, 19999).astype(jnp.int32),
    }


def normalize(counts, library):
    factor = 10000.0 / library.astype(jnp.float32)
    return jnp.log1p(counts.astype(jnp.float32) * factor[:, None]).astype(jnp.bfloat16)

def reference(counts, library):
    count_blocks = counts.reshape(N_CELLS, CELLS_DEV, G)
    library_blocks = library.reshape(N_CELLS, CELLS_DEV)

    def accumulate(carry, inputs):
        gram, sums, squares = carry
        expressed = normalize(inputs[0], inputs[1]).astype(jnp.float32)
        gram = gram + jnp.dot(expressed.T, expressed, precision=lax.Precision.HIGHEST, preferred_element_type=jnp.float32)
        sums = sums + lax.optimization_barrier(jnp.sum(expressed, axis=0))
        squares = squares + lax.optimization_barrier(jnp.sum(expressed * expressed, axis=0))
        return ((gram, sums, squares), None)
    start = (jnp.zeros((G, G), jnp.float32), jnp.zeros((G,), jnp.float32), jnp.zeros((G,), jnp.float32))
    (gram, sums, squares), unused = lax.scan(accumulate, start, (count_blocks, library_blocks))
    total_cells = float(CELLS)
    means = sums / total_cells
    variances = squares / total_cells - means * means
    scales = lax.rsqrt(variances + 1e-05)
    correlation = (gram / total_cells - means[:, None] * means[None, :]) * scales[:, None] * scales[None, :]
    powered = correlation ** 6
    diagonal = jnp.arange(G)[:, None] == jnp.arange(G)[None, :]
    adjacency = jnp.where(diagonal, jnp.float32(0.0), powered)
    connectivity = lax.optimization_barrier(jnp.sum(adjacency, axis=1))
    return (adjacency, connectivity)
```

```python
import functools

import jax
import jax.numpy as jnp
from jax import lax
from jax.experimental import pallas as pl
from jax.experimental.pallas import tpu as pltpu
from jax.sharding import PartitionSpec as P

CHUNKS = 8
TILE = 512
QUARTERS = 4
UNIT = 28000.0
MESH = pl.DeviceIdType.MESH


def bit(value, index):
    return (value // (1 << index)) % 2


def flip(value, index):
    return value + (1 << index) * (1 - 2 * bit(value, index))


def planes(own, sums_ref, out_ref, conn_ref,
           sib, stat, stream, tiles, land1, land2, outn, outt, inbox,
           pstat, message, table, columns, lanes, cmsg, cin,
           stat_send, stat_recv, side_send, sib_send, sib_recv, stream_send, stream_recv, go,
           one_send, one_recv, two_send, two_recv, norm_send, turn_send, in_recv,
           sum_send, sum_recv, row_send, row_recv, conn_send, conn_recv):
    quarters, width, cells = own.shape
    block = quarters * width
    total_cells = float(cells * 8)
    c = lax.axis_index("cells")
    g = lax.axis_index("genes")
    chip = c // 2
    core = c % 2
    side = g // 2
    far = 3 * side
    near = 1 + side
    beyond = 2 - side
    farther = 3 - 3 * side
    pair = g + 1 - 2 * (g % 2)
    other = c + 1 - 2 * core
    inner = (g == 1) | (g == 2)
    outer = (g == 0) | (g == 3)
    lead = core == side
    aux = core != side

    barrier = pltpu.get_barrier_semaphore()

    @pl.loop(1, 32)
    def _(d):
        t = lax.rem(c * 4 + g + d, 32)
        pl.semaphore_signal(barrier, inc=1, device_id=(t // 4, lax.rem(t, 4)), device_id_type=MESH)

    def remote(src, dst, send, recv, device):
        return pltpu.make_async_remote_copy(
            src_ref=src, dst_ref=dst, send_sem=send, recv_sem=recv, device_id=device, device_id_type=MESH)

    def swap(q):
        return remote(own.at[q], stat.at[q], stat_send.at[q], stat_recv.at[q], (c, pair))

    def share():
        return remote(own, sib, sib_send, sib_recv, (other, g))

    def back(q):
        return remote(own.at[q], stream.at[q], side_send.at[q], stream_recv.at[q], (other, far))

    def across(q):
        return remote(own.at[q], stream.at[q], stream_send.at[q], stream_recv.at[q], (c, beyond))

    def inward(q):
        return remote(own.at[q], stream.at[4 + q], stream_send.at[q], stream_recv.at[4 + q], (c, near))

    def relay(q):
        return remote(stream.at[4 + q], stream.at[4 + q], stream_send.at[4 + q], stream_recv.at[4 + q], (c, beyond))

    def local_sums(d):
        return remote(sums_ref, pstat.at[c], sum_send.at[d], sum_recv.at[c], (lax.rem(c + d, 8), g))

    def sums_from(d):
        source = lax.rem(c + d, 8)
        return remote(sums_ref, pstat.at[source], sum_send.at[d], sum_recv.at[source], (source, g))

    def genes_to(d):
        return remote(message, table.at[g], row_send.at[d], row_recv.at[g], (c, lax.rem(g + d, 4)))

    def genes_from(d):
        source = lax.rem(g + d, 4)
        return remote(message, table.at[source], row_send.at[d], row_recv.at[source], (c, source))

    def conn_to(d):
        return remote(cmsg, cin.at[g], conn_send.at[d], conn_recv.at[g], (c, lax.rem(g + d, 4)))

    def conn_from(d):
        source = lax.rem(g + d, 4)
        return remote(cmsg, cin.at[source], conn_send.at[d], conn_recv.at[source], (c, source))

    crossing = chip // 2 != side

    @pl.when(chip // 2 == side)
    def _():
        inbox[1 - side] = jnp.zeros(inbox.shape[1:], inbox.dtype)

    pl.semaphore_wait(barrier, 31)

    for d in range(1, 8):
        local_sums(d).start()

    @pl.when(lead)
    def _():
        swap(0).start()

    @pl.when(aux)
    def _():
        share().start()

    @pl.when(aux & inner)
    def _():
        across(0).start()
        back(0).start()

    pstat[c] = sums_ref[...]
    for d in range(1, 8):
        sums_from(d).wait_recv()
    everyone = pstat[0]
    for d in range(1, 8):
        everyone = everyone + pstat[d]
    together = pstat[2 * chip] + pstat[2 * chip + 1]
    means = everyone[0:1] / total_cells
    variances = everyone[1:2] / total_cells - means * means
    scales = lax.rsqrt(variances + 1e-05)
    message[0:1] = means
    message[1:2] = scales * ((UNIT / total_cells) ** 0.5)
    message[2:3] = sums_ref[0:1]
    message[3:4] = together[0:1]
    message[4:8] = jnp.zeros((4, block), jnp.float32)
    table[g] = message[...]
    for d in range(1, 4):
        genes_to(d).start()

    @pl.when(lead)
    def _():
        for q in range(1, 4):
            swap(q).start()

    @pl.when(aux & inner)
    def _():
        for q in range(1, 4):
            across(q).start()
            back(q).start()

    @pl.when(lead & outer)
    def _():
        for q in range(4):
            swap(q).wait_send()
        pl.semaphore_signal(go, inc=1, device_id=(other, g), device_id_type=MESH)

    @pl.when(aux & outer)
    def _():
        pl.semaphore_wait(go, 1)
        for q in range(4):
            inward(q).start()

    for d in range(1, 4):
        genes_from(d).wait_recv()

    @pl.when(aux & inner)
    def _():
        for q in range(4):
            inward(q).wait_recv()
            relay(q).start()

    def first_axis(idx):
        return 1 + idx % 2

    def turn(value, step):
        return value + step * (1 - 2 * ((value // step) % 2))

    def place(piece, idx):
        one = first_axis(idx)
        two = 3 - one
        return (2 * ((piece // one + chip // one) % 2) + (piece // two + chip // two) % 2)

    def fold_one(idx):
        partner = turn(chip, first_axis(idx))
        return remote(tiles.at[idx, pl.ds(2, 2)], land1.at[idx], one_send.at[idx], one_recv.at[idx],
                      (2 * partner + core, g))

    def fold_two(idx):
        partner = turn(chip, 3 - first_axis(idx))
        return remote(tiles.at[idx, 1], land2.at[idx], two_send.at[idx], two_recv.at[idx],
                      (2 * partner + core, g))

    def where(test, yes, no):
        return jnp.where(test, yes, no)

    late = lambda idx: (idx - 8) // 3
    phase = lambda idx: (idx - 8) % 3

    def rows_of(idx):
        crossed = where(idx < 8, beyond, where(phase(idx) == 0, beyond, farther))
        return where(inner, where(idx < 4, near, crossed), far)

    def quarter_of(idx):
        return where(inner & (idx >= 8), late(idx), idx % 4)

    def cols_of(idx):
        crossed = where(idx < 8, near, where(phase(idx) == 1, near, far))
        return where(inner, where(idx < 4, near, crossed), where(idx < 4, far, near))

    def normal(idx):
        q = quarter_of(idx)
        return remote(outn.at[idx], inbox.at[side, q % 2, chip], norm_send.at[idx], in_recv.at[side, q % 2, chip],
                      (2 * rows_of(idx) + q // 2, cols_of(idx)))

    def turned(idx):
        q = quarter_of(idx)
        return remote(outt.at[idx], inbox.at[side, chip % 2, q], turn_send.at[idx], in_recv.at[side, chip % 2, q],
                      (2 * cols_of(idx) + chip // 2, rows_of(idx)))

    def normal_here(idx):
        return (2 * rows_of(idx) + quarter_of(idx) // 2 == c) & (cols_of(idx) == g)

    def turned_here(idx):
        return (2 * cols_of(idx) + chip // 2 == c) & (rows_of(idx) == g)

    def absorb_one(idx):
        fold_one(idx).wait_recv()
        tiles[idx, 1] = (tiles[idx, 1].astype(jnp.int32) + land1[idx, 1].astype(jnp.int32)).astype(jnp.int16)
        fold_two(idx).start()

    def absorb_two(idx):
        fold_two(idx).wait_recv()
        total = (tiles[idx, 0].astype(jnp.int32) + land1[idx, 0].astype(jnp.int32)
                 + land2[idx].astype(jnp.int32))
        q = quarter_of(idx)
        here = normal_here(idx)

        @pl.when(here)
        def _():
            inbox[side, q % 2, chip] = total.astype(jnp.int16)

        @pl.when(jnp.logical_not(here))
        def _():
            outn[idx] = total.astype(jnp.int16)
            normal(idx).start()

        @pl.when(rows_of(idx) != cols_of(idx))
        def _():
            across_total = jnp.transpose(total)
            self_turned = turned_here(idx)

            @pl.when(self_turned)
            def _():
                inbox[side, chip % 2, q] = across_total.astype(jnp.int16)

            @pl.when(jnp.logical_not(self_turned))
            def _():
                outt[idx] = across_total.astype(jnp.int16)
                turned(idx).start()

    def product(idx, row, count, parts):
        row_block = rows_of(idx)
        col_block = cols_of(idx)
        first = pl.multiple_of(quarter_of(idx) * width, width)
        stats = columns[row_block, pl.ds(first, width), :]
        scale_j = stats[:, 1:2]
        mean_j = scale_j * stats[:, 0:1]
        sum_j = scale_j * stats[:, row:row + 1]

        @pl.loop(0, quarters)
        def _(p):
            acc = 0.0
            for left, right in parts:
                acc = acc + lax.dot_general(left[...], right(p)[...], (((1,), (1,)), ((), ())),
                                            preferred_element_type=jnp.float32)
            span = pl.ds(pl.multiple_of(p * width, width), width)
            mean_i = table[col_block, 0:1, span]
            scale_i = table[col_block, 1:2, span]
            drift_i = table[col_block, row:row + 1, span] - count * mean_i
            value = (acc * scale_j - mean_j * drift_i - sum_j * mean_i) * scale_i
            tiles[idx, place(p, idx)] = jnp.round(value).astype(jnp.int32).astype(jnp.int16)

    tasks = where(inner, 20, 8)

    @pl.when(lead)
    def _():
        for z in range(4):
            columns[z] = jnp.transpose(table[z])
        share().wait_recv()

        @pl.loop(0, tasks)
        def _(idx):
            q = quarter_of(idx)

            @pl.when(idx < 4)
            def _():
                product(idx, 3, 2.0 * cells,
                        [(own.at[q], lambda p: own.at[p]), (sib.at[q], lambda p: sib.at[p])])

            @pl.when(outer & (idx >= 4))
            def _():
                @pl.when(idx == 4)
                def _():
                    for t in range(4):
                        swap(t).wait_recv()
                        back(t).wait_recv()
                product(idx, 3, 2.0 * cells,
                        [(own.at[q], lambda p: stat.at[p]), (sib.at[q], lambda p: stream.at[p])])

            @pl.when(inner & (idx >= 4))
            def _():
                arriving = where(idx < 8, idx - 4, 4 + late(idx))
                waits = (idx < 8) | (phase(idx) == 1)

                @pl.when(waits)
                def _():
                    remote(own.at[0], stream.at[arriving], stream_send.at[arriving], stream_recv.at[arriving],
                           (c, beyond)).wait_recv()
                    product(idx, 2, 1.0 * cells, [(stream.at[arriving], lambda p: own.at[p])])

                @pl.when(jnp.logical_not(waits))
                def _():
                    @pl.when(idx == 8)
                    def _():
                        for t in range(4):
                            swap(t).wait_recv()
                    held = where(phase(idx) == 0, late(idx), 4 + late(idx))
                    product(idx, 2, 1.0 * cells, [(stream.at[held], lambda p: stat.at[p])])

            fold_one(idx).start()

            @pl.when(idx >= 1)
            def _():
                absorb_one(idx - 1)

            @pl.when(idx >= 2)
            def _():
                absorb_two(idx - 2)

        absorb_one(tasks - 1)
        absorb_two(tasks - 2)
        absorb_two(tasks - 1)

    lanes[...] = jnp.zeros_like(lanes)
    height = 2 * width

    @pl.loop(0, 8)
    def _(n):
        piece = n // 2
        r = n % 2
        mine = jnp.where(crossing, inner & (chip == piece),
                         jnp.where(chip == g, chip == piece, outer & (chip == 2 * core + r)))

        @pl.when(jnp.logical_not(mine & lead))
        def _():
            remote(outn.at[0], inbox.at[side, r, piece], norm_send.at[0], in_recv.at[side, r, piece],
                   (other, g)).wait_recv()

        @pl.when(crossing)
        def _():
            remote(outn.at[0], inbox.at[1 - side, r, piece], norm_send.at[0], in_recv.at[1 - side, r, piece],
                   (other, g)).wait_recv()
        total = inbox[0, r, piece].astype(jnp.int32) + inbox[1, r, piece].astype(jnp.int32)
        value = total.astype(jnp.float32) * (1.0 / UNIT)
        square = value * value
        powered = square * square * square
        rows = c * height + r * width + lax.broadcasted_iota(jnp.int32, (width, width), 0)
        cols = g * block + piece * width + lax.broadcasted_iota(jnp.int32, (width, width), 1)
        powered = jnp.where(rows == cols, 0.0, powered)
        down = pl.ds(pl.multiple_of(r * width, width), width)
        out_ref[down, pl.ds(pl.multiple_of(piece * width, width), width)] = powered
        part = powered[:, 0:128]
        for lane in range(1, width // 128):
            part = part + powered[:, lane * 128:(lane + 1) * 128]
        lanes[down, :] = lanes[down, :] + part

    cmsg[...] = jnp.broadcast_to(jnp.sum(jnp.transpose(lanes[...]), axis=0, keepdims=True), cmsg.shape)
    for d in range(1, 4):
        conn_to(d).start()
    cin[g] = cmsg[...]
    for d in range(1, 4):
        conn_from(d).wait_recv()
    conn_ref[...] = (cin[0] + cin[1]) + (cin[2] + cin[3])

    for d in range(1, 8):
        local_sums(d).wait_send()
    for d in range(1, 4):
        genes_to(d).wait_send()
        conn_to(d).wait_send()

    @pl.when(aux)
    def _():
        share().wait_send()

    @pl.when(aux & inner)
    def _():
        for q in range(4):
            across(q).wait_send()
            back(q).wait_send()
            relay(q).wait_send()

    @pl.when(aux & outer)
    def _():
        for q in range(4):
            inward(q).wait_send()

    @pl.when(lead & inner)
    def _():
        for q in range(4):
            swap(q).wait_send()

    @pl.when(lead)
    def _():
        @pl.loop(0, tasks)
        def _(idx):
            fold_one(idx).wait_send()
            fold_two(idx).wait_send()

            @pl.when(jnp.logical_not(normal_here(idx)))
            def _():
                normal(idx).wait_send()

            @pl.when((rows_of(idx) != cols_of(idx)) & jnp.logical_not(turned_here(idx)))
            def _():
                turned(idx).wait_send()


def by_planes(counts, library):
    factor = 10000.0 / library.astype(jnp.float32)
    expressed = jnp.log1p(counts.astype(jnp.float32) * factor[:, None])
    expressed = lax.reduce_precision(expressed, 8, 7)
    cells, block = expressed.shape
    width = block // QUARTERS
    sums = jnp.stack([jnp.sum(expressed, axis=0), jnp.sum(expressed * expressed, axis=0)])
    sums = jnp.concatenate([sums, jnp.zeros((6, block), jnp.float32)], axis=0)
    own = expressed.astype(jnp.bfloat16).T.reshape(QUARTERS, width, cells)
    vmem = pl.BlockSpec(memory_space=pltpu.VMEM)
    dma = pltpu.SemaphoreType.DMA
    small = jnp.int16
    count = 20
    adjacency, connectivity = pl.pallas_call(
        planes,
        out_shape=(
            jax.ShapeDtypeStruct((2 * width, block), jnp.float32),
            jax.ShapeDtypeStruct((8, 2 * width), jnp.float32),
        ),
        in_specs=[vmem] * 2,
        out_specs=(vmem, vmem),
        scratch_shapes=[
            pltpu.VMEM((QUARTERS, width, cells), jnp.bfloat16),
            pltpu.VMEM((QUARTERS, width, cells), jnp.bfloat16),
            pltpu.VMEM((8, width, cells), jnp.bfloat16),
            pltpu.VMEM((count, 4, width, width), small),
            pltpu.VMEM((count, 2, width, width), small),
            pltpu.VMEM((count, width, width), small),
            pltpu.VMEM((count, width, width), small),
            pltpu.VMEM((count, width, width), small),
            pltpu.VMEM((2, 2, 4, width, width), small),
            pltpu.VMEM((8, 8, block), jnp.float32),
            pltpu.VMEM((8, block), jnp.float32),
            pltpu.VMEM((4, 8, block), jnp.float32),
            pltpu.VMEM((4, block, 8), jnp.float32),
            pltpu.VMEM((2 * width, 128), jnp.float32),
            pltpu.VMEM((8, 2 * width), jnp.float32),
            pltpu.VMEM((4, 8, 2 * width), jnp.float32),
            dma((4,)), dma((4,)), dma((4,)), dma, dma, dma((8,)), dma((8,)), pltpu.SemaphoreType.REGULAR,
            dma((count,)), dma((count,)), dma((count,)), dma((count,)), dma((count,)), dma((count,)), dma((2, 2, 4)),
            dma((8,)), dma((8,)), dma((4,)), dma((4,)), dma((4,)), dma((4,)),
        ],
        compiler_params=pltpu.CompilerParams(
            collective_id=1, has_side_effects=True, vmem_limit_bytes=58 * 1024 * 1024),
    )(own, sums)
    return adjacency, connectivity[0]


def network(cell_groups, gene_groups, xq_ref, own_ref, sums_ref, out_ref, stats_ref,
            held, partial, landed, totals, sums_in,
            ring_send, ring_recv, cut_send, cut_recv, fly_send, fly_recv, stat_send, stat_recv):
    owners, chunks, part, cells = xq_ref.shape
    rows = owners * part
    cols = own_ref.shape[1]
    half = cols // 2
    c = lax.axis_index("cells")
    g = lax.axis_index("genes")
    right = lax.rem(g + 1, gene_groups)
    left = lax.rem(g + gene_groups - 1, gene_groups)
    bits = cell_groups.bit_length() - 1
    hops = gene_groups - 1
    orders = (tuple(range(bits)), (0,) + tuple(range(bits - 1, 0, -1)))

    barrier = pltpu.get_barrier_semaphore()
    for target in [(c, left), (c, right)] + [(flip(c, b), g) for b in range(bits)]:
        pl.semaphore_signal(barrier, inc=1, device_id=target, device_id_type=pl.DeviceIdType.MESH)
    pl.semaphore_wait(barrier, 2 + bits)

    def ring(q, hop, piece):
        span = pl.ds(piece * (owners // 2), owners // 2)
        source = xq_ref.at[span, q] if hop == 0 else held.at[q, hop - 1, span]
        return pltpu.make_async_remote_copy(
            src_ref=source, dst_ref=held.at[q, hop, span],
            send_sem=ring_send.at[q, hop, piece], recv_sem=ring_recv.at[q, hop, piece],
            device_id=(c, right), device_id_type=pl.DeviceIdType.MESH)

    def cut(q, side, stage):
        count = cell_groups >> (stage + 1)
        return pltpu.make_async_remote_copy(
            src_ref=partial.at[q, side, pl.ds(count, count)],
            dst_ref=landed.at[q, side, pl.ds(count, count)],
            send_sem=cut_send.at[q, side, stage], recv_sem=cut_recv.at[q, side, stage],
            device_id=(flip(c, orders[side][stage]), g), device_id_type=pl.DeviceIdType.MESH)

    def fly(stage):
        return pltpu.make_async_remote_copy(
            src_ref=totals.at[stage], dst_ref=sums_in.at[stage],
            send_sem=fly_send.at[stage], recv_sem=fly_recv.at[stage],
            device_id=(flip(c, stage), g), device_id_type=pl.DeviceIdType.MESH)

    def spread(hop):
        source = totals.at[bits] if hop == 0 else stats_ref.at[hop]
        return pltpu.make_async_remote_copy(
            src_ref=source, dst_ref=stats_ref.at[hop + 1],
            send_sem=stat_send.at[hop], recv_sem=stat_recv.at[hop],
            device_id=(c, right), device_id_type=pl.DeviceIdType.MESH)

    def place(owner, side):
        total = 0
        for position, b in enumerate(orders[side]):
            total = total + ((bit(owner, b) + bit(c, b)) % 2) * (1 << (bits - 1 - position))
        return total

    def multiply(q, step):
        source = lax.rem(g - step + gene_groups, gene_groups)
        block = xq_ref.at[:, q] if step == 0 else held.at[q, step - 1]
        for side in range(2):
            spots = [place(source * owners + o, side) for o in range(owners)]

            @pl.loop(0, half // TILE)
            def _(t):
                start = pl.multiple_of(t * TILE, TILE)
                columns = pl.ds(pl.multiple_of(side * half + start, TILE), TILE)
                tile = jnp.dot(block[...].reshape(rows, cells), own_ref[:, columns], preferred_element_type=jnp.float32)
                for o in range(owners):
                    partial[q, side, spots[o], :, pl.ds(start, TILE)] = tile[o * part:(o + 1) * part]

    def launch(q, stage):
        for side in range(2):
            cut(q, side, stage).start()

    def absorb(q, stage):
        count = cell_groups >> (stage + 1)
        for side in range(2):
            cut(q, side, stage).wait_recv()
            if count > 1:
                @pl.loop(0, count)
                def _(i):
                    partial[q, side, i] = partial[q, side, i] + landed[q, side, i + count]
            else:
                out_ref[pl.ds(q * part, part), side * half:(side + 1) * half] = (
                    partial[q, side, 0] + landed[q, side, 1])

    for piece in range(2):
        ring(0, 0, piece).start()
    totals[0] = sums_ref[...]
    for stage in range(bits):
        fly(stage).start()
        fly(stage).wait_recv()
        totals[stage + 1] = totals[stage] + sums_in[stage]
    stats_ref[0] = totals[bits]

    turns = [[s for s in range(bits) if s * hops // bits == h] for h in range(hops)]

    @pl.loop(0, chunks)
    def _(q):
        multiply(q, 0)
        for hop in range(hops):
            for piece in range(2):
                ring(q, hop, piece).wait_recv()
                if hop < hops - 1:
                    ring(q, hop + 1, piece).start()
            if hop == max(hops - 2, 0):
                @pl.when(q < chunks - 1)
                def _():
                    for piece in range(2):
                        ring(q + 1, 0, piece).start()

            @pl.when(q > 0)
            def _():
                for stage in turns[hop]:
                    absorb(q - 1, stage)
                    if stage + 1 < bits:
                        launch(q - 1, stage + 1)
            multiply(q, hop + 1)
        launch(q, 0)

    last = chunks - 1
    spread(0).start()
    for stage in range(bits):
        absorb(last, stage)
        if stage + 1 < bits:
            launch(last, stage + 1)
        if stage < hops:
            spread(stage).wait_recv()
            if stage + 1 < hops:
                spread(stage + 1).start()
    for hop in range(bits, hops):
        spread(hop).wait_recv()
        if hop + 1 < hops:
            spread(hop + 1).start()
    for hop in range(hops):
        spread(hop).wait_send()
    for stage in range(bits):
        fly(stage).wait_send()

    @pl.loop(0, chunks)
    def _(q):
        for hop in range(hops):
            for piece in range(2):
                ring(q, hop, piece).wait_send()
        for side in range(2):
            for stage in range(bits):
                cut(q, side, stage).wait_send()


def normalize(counts, library):
    factor = 10000.0 / library.astype(jnp.float32)
    return jnp.log1p(counts.astype(jnp.float32) * factor[:, None]).astype(jnp.bfloat16)


def shards(counts, library):
    own_block = normalize(counts, library)
    cells, col_width = own_block.shape
    cell_groups = lax.axis_size("cells")
    gene_groups = lax.axis_size("genes")
    row_width = col_width * gene_groups // cell_groups
    owners = col_width // row_width
    total_cells = float(cells * cell_groups)
    me = lax.axis_index("genes")

    chunks = min(CHUNKS, row_width // 16)
    part = row_width // chunks
    ordered = own_block.T.reshape(owners, chunks, part, cells)
    widened = own_block.astype(jnp.float32)
    sums = jnp.stack([jnp.sum(widened, axis=0), jnp.sum(widened * widened, axis=0)])
    sums = jnp.concatenate([sums, jnp.zeros((6, col_width), jnp.float32)], axis=0)
    bits = cell_groups.bit_length() - 1
    hops = gene_groups - 1
    vmem = pl.BlockSpec(memory_space=pltpu.VMEM)
    dma = pltpu.SemaphoreType.DMA
    gram_tile, stats = pl.pallas_call(
        functools.partial(network, cell_groups, gene_groups),
        out_shape=(
            jax.ShapeDtypeStruct((row_width, col_width), jnp.float32),
            jax.ShapeDtypeStruct((gene_groups, 8, col_width), jnp.float32),
        ),
        in_specs=[vmem] * 3,
        out_specs=(vmem, vmem),
        scratch_shapes=[
            pltpu.VMEM((chunks, hops, owners, part, cells), jnp.bfloat16),
            pltpu.VMEM((chunks, 2, cell_groups, part, col_width // 2), jnp.float32),
            pltpu.VMEM((chunks, 2, cell_groups, part, col_width // 2), jnp.float32),
            pltpu.VMEM((bits + 1, 8, col_width), jnp.float32),
            pltpu.VMEM((bits, 8, col_width), jnp.float32),
            dma((chunks, hops, 2)), dma((chunks, hops, 2)),
            dma((chunks, 2, bits)), dma((chunks, 2, bits)),
            dma((bits,)), dma((bits,)),
            dma((hops,)), dma((hops,)),
        ],
        compiler_params=pltpu.CompilerParams(
            collective_id=0, has_side_effects=True, vmem_limit_bytes=60 * 1024 * 1024),
    )(ordered, own_block, sums)
    order = lax.rem(me - jnp.arange(gene_groups) + gene_groups, gene_groups)
    all_sums = jnp.transpose(jnp.take(stats[:, :2], order, axis=0), (1, 0, 2)).reshape(2, -1)

    means = all_sums[0] / total_cells
    variances = all_sums[1] / total_cells - means * means
    scales = lax.rsqrt(variances + 1e-05)
    row_first = lax.axis_index("cells") * row_width
    col_first = me * col_width
    row_means = lax.dynamic_slice_in_dim(means, row_first, row_width, 0)
    col_means = lax.dynamic_slice_in_dim(means, col_first, col_width, 0)
    row_scales = lax.dynamic_slice_in_dim(scales, row_first, row_width, 0)
    col_scales = lax.dynamic_slice_in_dim(scales, col_first, col_width, 0)
    correlation = (
        (gram_tile / total_cells - row_means[:, None] * col_means[None, :])
        * row_scales[:, None]
        * col_scales[None, :]
    )
    powered = correlation**6
    row_index = row_first + jnp.arange(row_width, dtype=jnp.int32)[:, None]
    col_index = col_first + jnp.arange(col_width, dtype=jnp.int32)[None, :]
    adjacency = jnp.where(row_index == col_index, jnp.float32(0.0), powered)
    connectivity = lax.psum(jnp.sum(adjacency, axis=1), "genes")
    return (adjacency, connectivity)


def solution(mesh):
    sized = mesh.shape["genes"] == 4 and mesh.shape["cells"] == 8
    return jax.shard_map(
        by_planes if sized else shards,
        mesh=mesh,
        in_specs=(P("cells", "genes"), P("cells")),
        out_specs=(P("cells", "genes"), P("cells")),
        check_vma=False,
    )
```

```python
import functools

import jax
import jax.numpy as jnp
from jax import lax
from jax.experimental import pallas as pl
from jax.experimental.pallas import tpu as pltpu
from jax.sharding import PartitionSpec as P

CHUNKS = 8
TILE = 512
QUARTERS = 4
UNIT = 28000.0
LAG_ONE = 3
LAG_TWO = 5
GO_AT = 6
MESH = pl.DeviceIdType.MESH


def bit(value, index):
    return (value // (1 << index)) % 2


def flip(value, index):
    return value + (1 << index) * (1 - 2 * bit(value, index))


def planes(counts_ref, library_ref, out_ref, conn_ref,
           raw, own, sums_ref, squares, result, sib, stat, held, stream, tiles, land1, land2, whole, outn, outt, inbox,
           pstat, message, table, columns, lanes, cmsg, cin,
           stat_send, stat_recv, held_send, held_recv, sib_send, sib_recv, stream_send, stream_recv, go,
           one_send, one_recv, two_send, two_recv, hand_send, hand_recv, norm_send, turn_send, in_recv,
           load_done, store_done, sum_send, sum_recv, row_send, row_recv, conn_send, conn_recv):
    quarters, width, cells = own.shape
    total_cells = float(cells * 8)
    c = lax.axis_index("cells")
    g = lax.axis_index("genes")
    chip = c // 2
    core = c % 2
    side = g // 2
    far = 3 * side
    near = 1 + side
    beyond = 2 - side
    farther = 3 - 3 * side
    other = c + 1 - 2 * core
    inner = (g == 1) | (g == 2)
    outer = (g == 0) | (g == 3)
    lead = core == side
    aux = core != side

    barrier = pltpu.get_barrier_semaphore()

    @pl.loop(1, 32)
    def _(d):
        t = lax.rem(c * 4 + g + d, 32)
        pl.semaphore_signal(barrier, inc=1, device_id=(t // 4, lax.rem(t, 4)), device_id_type=MESH)

    slabs, slab, block = raw.shape

    def load(r):
        return pltpu.make_async_copy(counts_ref.at[pl.ds(r * slab, slab)], raw.at[r], load_done.at[r])

    @pl.loop(0, slabs)
    def _(r):
        load(r).start()

    sums_ref[...] = jnp.zeros_like(sums_ref)
    squares[...] = jnp.zeros_like(squares)

    @pl.loop(0, slabs)
    def _(r):
        load(r).wait()
        factor = 10000.0 / library_ref[pl.ds(r, 1), :].astype(jnp.float32)
        factor = jnp.transpose(jnp.broadcast_to(factor, (8, slab)))[:, 0:1]
        expressed = jnp.log1p(raw[r].astype(jnp.float32) * factor).astype(jnp.bfloat16).astype(jnp.float32)
        sums_ref[...] = sums_ref[...] + jnp.sum(expressed.reshape(slab // 8, 8, block), axis=0)
        squares[...] = squares[...] + jnp.sum((expressed * expressed).reshape(slab // 8, 8, block), axis=0)
        turned_slab = jnp.transpose(expressed).astype(jnp.bfloat16).reshape(quarters, width, slab)
        own[:, :, pl.ds(pl.multiple_of(r * slab, slab), slab)] = turned_slab

    total_sum = jnp.sum(sums_ref[...], axis=0, keepdims=True)
    total_square = jnp.sum(squares[...], axis=0, keepdims=True)
    sums_ref[...] = jnp.zeros_like(sums_ref)
    sums_ref[0:1] = total_sum
    sums_ref[1:2] = total_square

    def remote(src, dst, send, recv, device):
        return pltpu.make_async_remote_copy(
            src_ref=src, dst_ref=dst, send_sem=send, recv_sem=recv, device_id=device, device_id_type=MESH)

    def share():
        return remote(own, sib, sib_send, sib_recv, (other, g))

    def across(q):
        return remote(own.at[q], stream.at[q], stream_send.at[q], stream_recv.at[q], (c, beyond))

    def inward(q):
        return remote(own.at[q], stream.at[4 + q], stream_send.at[q], stream_recv.at[4 + q], (c, near))

    def relay(q):
        return remote(stream.at[4 + q], stream.at[4 + q], stream_send.at[4 + q], stream_recv.at[4 + q], (c, beyond))

    def beside(q):
        return remote(stream.at[4 + q], held.at[q], held_send.at[q], held_recv.at[q], (other, g))

    def onward(t):
        return remote(stream.at[t], stream.at[t], stream_send.at[t], stream_recv.at[t], (c, far))

    def swap(q):
        return remote(own.at[q], stat.at[q], stat_send.at[q], stat_recv.at[q], (c, near))

    def local_sums(d):
        return remote(sums_ref, pstat.at[c], sum_send.at[d], sum_recv.at[c], (lax.rem(c + d, 8), g))

    def sums_from(d):
        source = lax.rem(c + d, 8)
        return remote(sums_ref, pstat.at[source], sum_send.at[d], sum_recv.at[source], (source, g))

    def genes_to(d):
        return remote(message, table.at[g], row_send.at[d], row_recv.at[g], (c, lax.rem(g + d, 4)))

    def genes_from(d):
        source = lax.rem(g + d, 4)
        return remote(message, table.at[source], row_send.at[d], row_recv.at[source], (c, source))

    def conn_to(d):
        return remote(cmsg, cin.at[g], conn_send.at[d], conn_recv.at[g], (c, lax.rem(g + d, 4)))

    def conn_from(d):
        source = lax.rem(g + d, 4)
        return remote(cmsg, cin.at[source], conn_send.at[d], conn_recv.at[source], (c, source))

    crossing = chip // 2 != side

    @pl.when(chip // 2 == side)
    def _():
        inbox[1 - side] = jnp.zeros(inbox.shape[1:], inbox.dtype)

    pl.semaphore_wait(barrier, 31)

    for d in range(1, 8):
        local_sums(d).start()

    @pl.when(aux & inner)
    def _():
        across(0).start()

    @pl.when(aux & outer)
    def _():
        inward(0).start()

    @pl.when(aux)
    def _():
        share().start()

    pstat[c] = sums_ref[...]
    for d in range(1, 8):
        sums_from(d).wait_recv()
    everyone = pstat[0]
    for d in range(1, 8):
        everyone = everyone + pstat[d]
    together = pstat[2 * chip] + pstat[2 * chip + 1]
    means = everyone[0:1] / total_cells
    variances = everyone[1:2] / total_cells - means * means
    scales = lax.rsqrt(variances + 1e-05)
    message[0:1] = means
    message[1:2] = scales * ((UNIT / total_cells) ** 0.5)
    message[2:3] = sums_ref[0:1]
    message[3:4] = together[0:1]
    message[4:8] = jnp.zeros((4, block), jnp.float32)
    table[g] = message[...]
    for d in range(1, 4):
        genes_to(d).start()

    @pl.when(aux & inner)
    def _():
        for q in range(1, 4):
            across(q).start()
        for q in range(4):
            inward(q).wait_recv()
            relay(q).start()
            beside(q).start()

    @pl.when(aux & outer)
    def _():
        for q in range(1, 4):
            inward(q).start()
        for q in range(4):
            inward(q).wait_send()
        pl.semaphore_signal(go, inc=1, device_id=(other, g), device_id_type=MESH)

    @pl.when(aux)
    def _():
        for d in range(1, 4):
            genes_from(d).wait_recv()

    def where(test, yes, no):
        return jnp.where(test, yes, no)

    def first_axis(idx):
        return 1 + 0 * idx

    def turn(value, step):
        return value + step * (1 - 2 * ((value // step) % 2))

    def place(piece, idx):
        one = first_axis(idx)
        two = 3 - one
        return (2 * ((piece // one + chip // one) % 2) + (piece // two + chip // two) % 2)

    def fold_one(idx):
        partner = turn(chip, first_axis(idx))
        return remote(tiles.at[idx, pl.ds(2, 2)], land1.at[idx], one_send.at[idx], one_recv.at[idx],
                      (2 * partner + core, g))

    def fold_two(idx):
        partner = turn(chip, 3 - first_axis(idx))
        return remote(tiles.at[idx, 1], land2.at[idx], two_send.at[idx], two_recv.at[idx],
                      (2 * partner + core, g))

    def rows_of(idx):
        crossed = where(idx < 8, beyond, where(idx < 12, farther, far))
        return where(idx < 4, g, crossed)

    def hand(idx):
        return remote(whole.at[idx], outn.at[idx], hand_send.at[idx], hand_recv.at[idx], (other, g))

    def normal(idx):
        q = idx % 4
        return remote(outn.at[idx], inbox.at[side, q % 2, chip], norm_send.at[idx], in_recv.at[side, q % 2, chip],
                      (2 * rows_of(idx) + q // 2, g))

    def turned(idx):
        q = idx % 4
        return remote(outt.at[idx], inbox.at[side, chip % 2, q], turn_send.at[idx], in_recv.at[side, chip % 2, q],
                      (2 * g + chip // 2, rows_of(idx)))

    def normal_here(idx):
        return 2 * rows_of(idx) + (idx % 4) // 2 == c

    def absorb_one(idx):
        fold_one(idx).wait_recv()
        tiles[idx, 1] = (tiles[idx, 1].astype(jnp.int32) + land1[idx, 1].astype(jnp.int32)).astype(jnp.int16)
        fold_two(idx).start()

    def absorb_two(idx):
        fold_two(idx).wait_recv()
        total = (tiles[idx, 0].astype(jnp.int32) + land1[idx, 0].astype(jnp.int32)
                 + land2[idx].astype(jnp.int32))
        whole[idx] = total.astype(jnp.int16)
        hand(idx).start()

    def deliver(idx):
        hand(idx).wait_recv()
        q = idx % 4
        here = normal_here(idx)

        @pl.when(here)
        def _():
            inbox[side, q % 2, chip] = outn[idx]

        @pl.when(jnp.logical_not(here))
        def _():
            normal(idx).start()

        @pl.when(idx >= 4)
        def _():
            outt[idx] = jnp.transpose(outn[idx].astype(jnp.int32)).astype(jnp.int16)
            turned(idx).start()

    def product(idx, row, count, parts):
        row_block = rows_of(idx)
        col_block = g
        first = pl.multiple_of((idx % 4) * width, width)
        stats = columns[row_block, pl.ds(first, width), :]
        scale_j = stats[:, 1:2]
        mean_j = scale_j * stats[:, 0:1]
        sum_j = scale_j * stats[:, row:row + 1]

        @pl.loop(0, quarters)
        def _(p):
            acc = 0.0
            for left, right in parts:
                acc = acc + lax.dot_general(left[...], right(p)[...], (((1,), (1,)), ((), ())),
                                            preferred_element_type=jnp.float32)
            span = pl.ds(pl.multiple_of(p * width, width), width)
            mean_i = table[col_block, 0:1, span]
            scale_i = table[col_block, 1:2, span]
            drift_i = table[col_block, row:row + 1, span] - count * mean_i
            value = (acc * scale_j - mean_j * drift_i - sum_j * mean_i) * scale_i
            tiles[idx, place(p, idx)] = jnp.round(value).astype(jnp.int32).astype(jnp.int16)

    tasks = where(inner, 16, 12)

    def step(idx):
        q = idx % 4

        @pl.when(idx == 4)
        def _():
            for d in range(1, 4):
                genes_from(d).wait_recv()
                z = lax.rem(g + d, 4)
                columns[z] = jnp.transpose(table[z])

        @pl.when(outer & (idx == GO_AT))
        def _():
            pl.semaphore_wait(go, 1)
            for t in range(4):
                swap(t).start()

        @pl.when(idx < 4)
        def _():
            product(idx, 3, 2.0 * cells,
                    [(own.at[q], lambda p: own.at[p]), (sib.at[q], lambda p: sib.at[p])])

        @pl.when((idx >= 4) & (idx < 12))
        def _():
            slot = idx - 4
            remote(own.at[0], stream.at[slot], stream_send.at[slot], stream_recv.at[slot], (c, beyond)).wait_recv()

            @pl.when(inner)
            def _():
                onward(slot).start()
            product(idx, 2, 1.0 * cells, [(stream.at[slot], lambda p: own.at[p])])

        @pl.when(idx >= 12)
        def _():
            swap(q).wait_recv()
            beside(q).wait_recv()
            product(idx, 3, 2.0 * cells,
                    [(stat.at[q], lambda p: own.at[p]), (held.at[q], lambda p: sib.at[p])])

        fold_one(idx).start()

    @pl.when(lead)
    def _():
        columns[g] = jnp.transpose(table[g])
        share().wait_recv()

        @pl.loop(0, tasks + LAG_TWO)
        def _(idx):
            @pl.when(idx < tasks)
            def _():
                step(idx)

            @pl.when((idx >= LAG_ONE) & (idx < tasks + LAG_ONE))
            def _():
                absorb_one(idx - LAG_ONE)

            @pl.when(idx >= LAG_TWO)
            def _():
                absorb_two(idx - LAG_TWO)

    @pl.when(aux)
    def _():
        pl.loop(0, tasks)(deliver)

    def store(r, piece):
        down = pl.ds(pl.multiple_of(r * width, width), width)
        along = pl.ds(pl.multiple_of(piece * width, width), width)
        return pltpu.make_async_copy(result.at[r, piece], out_ref.at[down, along], store_done.at[r, piece])

    lanes[...] = jnp.zeros_like(lanes)
    height = 2 * width

    @pl.loop(0, 8)
    def _(n):
        piece = n // 2
        r = n % 2
        mine = (chip == piece) & (crossing | (chip == g) | inner)

        @pl.when(jnp.logical_not(mine & aux))
        def _():
            remote(outn.at[0], inbox.at[side, r, piece], norm_send.at[0], in_recv.at[side, r, piece],
                   (other, g)).wait_recv()

        @pl.when(crossing)
        def _():
            remote(outn.at[0], inbox.at[1 - side, r, piece], norm_send.at[0], in_recv.at[1 - side, r, piece],
                   (other, g)).wait_recv()
        total = inbox[0, r, piece].astype(jnp.int32) + inbox[1, r, piece].astype(jnp.int32)
        result[r, piece] = total.astype(jnp.int16)
        store(r, piece).start()
        value = total.astype(jnp.float32) * (1.0 / UNIT)
        square = value * value
        powered = square * square * square
        rows = c * height + r * width + lax.broadcasted_iota(jnp.int32, (width, width), 0)
        cols = g * block + piece * width + lax.broadcasted_iota(jnp.int32, (width, width), 1)
        powered = jnp.where(rows == cols, 0.0, powered)
        down = pl.ds(pl.multiple_of(r * width, width), width)
        part = powered[:, 0:128]
        for lane in range(1, width // 128):
            part = part + powered[:, lane * 128:(lane + 1) * 128]
        lanes[down, :] = lanes[down, :] + part

    cmsg[...] = jnp.broadcast_to(jnp.sum(jnp.transpose(lanes[...]), axis=0, keepdims=True), cmsg.shape)
    for d in range(1, 4):
        conn_to(d).start()
    cin[g] = cmsg[...]
    for d in range(1, 4):
        conn_from(d).wait_recv()
    conn_ref[...] = ((cin[0] + cin[1]) + (cin[2] + cin[3]))[0:1]

    @pl.loop(0, 8)
    def _(n):
        store(n % 2, n // 2).wait()

    for d in range(1, 8):
        local_sums(d).wait_send()
    for d in range(1, 4):
        genes_to(d).wait_send()
        conn_to(d).wait_send()

    @pl.when(aux)
    def _():
        share().wait_send()

    @pl.when(aux & inner)
    def _():
        for q in range(4):
            across(q).wait_send()
            relay(q).wait_send()
            beside(q).wait_send()

    @pl.when(lead & outer)
    def _():
        for q in range(4):
            swap(q).wait_send()

    @pl.when(lead & inner)
    def _():
        for t in range(8):
            onward(t).wait_send()

    @pl.when(lead)
    def _():
        @pl.loop(0, tasks)
        def _(idx):
            fold_one(idx).wait_send()
            fold_two(idx).wait_send()
            hand(idx).wait_send()

    @pl.when(aux)
    def _():
        @pl.loop(0, tasks)
        def _(idx):
            @pl.when(jnp.logical_not(normal_here(idx)))
            def _():
                normal(idx).wait_send()

            @pl.when(idx >= 4)
            def _():
                turned(idx).wait_send()


def by_planes(counts, library):
    cells, block = counts.shape
    width = block // QUARTERS
    slab = 128
    vmem = pl.BlockSpec(memory_space=pltpu.VMEM)
    anywhere = pl.BlockSpec(memory_space=pl.ANY)
    dma = pltpu.SemaphoreType.DMA
    small = jnp.int16
    count = 16
    quarters = pltpu.VMEM((QUARTERS, width, cells), jnp.bfloat16)
    pieces = pltpu.VMEM((count, width, width), small)
    row = pltpu.VMEM((8, block), jnp.float32)
    totals, connectivity = pl.pallas_call(
        planes,
        out_shape=(
            jax.ShapeDtypeStruct((2 * width, block), small),
            jax.ShapeDtypeStruct((1, 2 * width), jnp.float32),
        ),
        in_specs=[anywhere, vmem],
        out_specs=(anywhere, vmem),
        scratch_shapes=[
            pltpu.VMEM((cells // slab, slab, block), jnp.int32),
            quarters, row, row,
            pltpu.VMEM((2, 4, width, width), small),
            quarters, quarters, quarters,
            pltpu.VMEM((8, width, cells), jnp.bfloat16),
            pltpu.VMEM((count, 4, width, width), small),
            pltpu.VMEM((count, 2, width, width), small),
            pieces, pieces, pieces, pieces,
            pltpu.VMEM((2, 2, 4, width, width), small),
            pltpu.VMEM((8, 8, block), jnp.float32),
            row,
            pltpu.VMEM((4, 8, block), jnp.float32),
            pltpu.VMEM((4, block, 8), jnp.float32),
            pltpu.VMEM((2 * width, 128), jnp.float32),
            pltpu.VMEM((8, 2 * width), jnp.float32),
            pltpu.VMEM((4, 8, 2 * width), jnp.float32),
            dma((4,)), dma((4,)), dma((4,)), dma((4,)), dma, dma, dma((8,)), dma((8,)), pltpu.SemaphoreType.REGULAR,
            dma((count,)), dma((count,)), dma((count,)), dma((count,)), dma((count,)), dma((count,)),
            dma((count,)), dma((count,)), dma((2, 2, 4)),
            dma((cells // slab,)), dma((2, 4)),
            dma((8,)), dma((8,)), dma((4,)), dma((4,)), dma((4,)), dma((4,)),
        ],
        compiler_params=pltpu.CompilerParams(
            collective_id=1, has_side_effects=True, vmem_limit_bytes=58 * 1024 * 1024),
    )(counts, library.reshape(cells // slab, slab))
    value = totals.astype(jnp.float32) * (1.0 / UNIT)
    square = value * value
    rows = lax.axis_index("cells") * 2 * width + jnp.arange(2 * width, dtype=jnp.int32)[:, None]
    cols = lax.axis_index("genes") * block + jnp.arange(block, dtype=jnp.int32)[None, :]
    adjacency = jnp.where(rows == cols, jnp.float32(0.0), square * square * square)
    return adjacency, connectivity.reshape(2 * width)


def network(cell_groups, gene_groups, xq_ref, own_ref, sums_ref, out_ref, stats_ref,
            held, partial, landed, totals, sums_in,
            ring_send, ring_recv, cut_send, cut_recv, fly_send, fly_recv, stat_send, stat_recv):
    owners, chunks, part, cells = xq_ref.shape
    rows = owners * part
    cols = own_ref.shape[1]
    half = cols // 2
    c = lax.axis_index("cells")
    g = lax.axis_index("genes")
    right = lax.rem(g + 1, gene_groups)
    left = lax.rem(g + gene_groups - 1, gene_groups)
    bits = cell_groups.bit_length() - 1
    hops = gene_groups - 1
    orders = (tuple(range(bits)), (0,) + tuple(range(bits - 1, 0, -1)))

    barrier = pltpu.get_barrier_semaphore()
    for target in [(c, left), (c, right)] + [(flip(c, b), g) for b in range(bits)]:
        pl.semaphore_signal(barrier, inc=1, device_id=target, device_id_type=pl.DeviceIdType.MESH)
    pl.semaphore_wait(barrier, 2 + bits)

    def ring(q, hop, piece):
        span = pl.ds(piece * (owners // 2), owners // 2)
        source = xq_ref.at[span, q] if hop == 0 else held.at[q, hop - 1, span]
        return pltpu.make_async_remote_copy(
            src_ref=source, dst_ref=held.at[q, hop, span],
            send_sem=ring_send.at[q, hop, piece], recv_sem=ring_recv.at[q, hop, piece],
            device_id=(c, right), device_id_type=pl.DeviceIdType.MESH)

    def cut(q, side, stage):
        count = cell_groups >> (stage + 1)
        return pltpu.make_async_remote_copy(
            src_ref=partial.at[q, side, pl.ds(count, count)],
            dst_ref=landed.at[q, side, pl.ds(count, count)],
            send_sem=cut_send.at[q, side, stage], recv_sem=cut_recv.at[q, side, stage],
            device_id=(flip(c, orders[side][stage]), g), device_id_type=pl.DeviceIdType.MESH)

    def fly(stage):
        return pltpu.make_async_remote_copy(
            src_ref=totals.at[stage], dst_ref=sums_in.at[stage],
            send_sem=fly_send.at[stage], recv_sem=fly_recv.at[stage],
            device_id=(flip(c, stage), g), device_id_type=pl.DeviceIdType.MESH)

    def spread(hop):
        source = totals.at[bits] if hop == 0 else stats_ref.at[hop]
        return pltpu.make_async_remote_copy(
            src_ref=source, dst_ref=stats_ref.at[hop + 1],
            send_sem=stat_send.at[hop], recv_sem=stat_recv.at[hop],
            device_id=(c, right), device_id_type=pl.DeviceIdType.MESH)

    def place(owner, side):
        total = 0
        for position, b in enumerate(orders[side]):
            total = total + ((bit(owner, b) + bit(c, b)) % 2) * (1 << (bits - 1 - position))
        return total

    def multiply(q, step):
        source = lax.rem(g - step + gene_groups, gene_groups)
        block = xq_ref.at[:, q] if step == 0 else held.at[q, step - 1]
        for side in range(2):
            spots = [place(source * owners + o, side) for o in range(owners)]

            @pl.loop(0, half // TILE)
            def _(t):
                start = pl.multiple_of(t * TILE, TILE)
                columns = pl.ds(pl.multiple_of(side * half + start, TILE), TILE)
                tile = jnp.dot(block[...].reshape(rows, cells), own_ref[:, columns], preferred_element_type=jnp.float32)
                for o in range(owners):
                    partial[q, side, spots[o], :, pl.ds(start, TILE)] = tile[o * part:(o + 1) * part]

    def launch(q, stage):
        for side in range(2):
            cut(q, side, stage).start()

    def absorb(q, stage):
        count = cell_groups >> (stage + 1)
        for side in range(2):
            cut(q, side, stage).wait_recv()
            if count > 1:
                @pl.loop(0, count)
                def _(i):
                    partial[q, side, i] = partial[q, side, i] + landed[q, side, i + count]
            else:
                out_ref[pl.ds(q * part, part), side * half:(side + 1) * half] = (
                    partial[q, side, 0] + landed[q, side, 1])

    for piece in range(2):
        ring(0, 0, piece).start()
    totals[0] = sums_ref[...]
    for stage in range(bits):
        fly(stage).start()
        fly(stage).wait_recv()
        totals[stage + 1] = totals[stage] + sums_in[stage]
    stats_ref[0] = totals[bits]

    turns = [[s for s in range(bits) if s * hops // bits == h] for h in range(hops)]

    @pl.loop(0, chunks)
    def _(q):
        multiply(q, 0)
        for hop in range(hops):
            for piece in range(2):
                ring(q, hop, piece).wait_recv()
                if hop < hops - 1:
                    ring(q, hop + 1, piece).start()
            if hop == max(hops - 2, 0):
                @pl.when(q < chunks - 1)
                def _():
                    for piece in range(2):
                        ring(q + 1, 0, piece).start()

            @pl.when(q > 0)
            def _():
                for stage in turns[hop]:
                    absorb(q - 1, stage)
                    if stage + 1 < bits:
                        launch(q - 1, stage + 1)
            multiply(q, hop + 1)
        launch(q, 0)

    last = chunks - 1
    spread(0).start()
    for stage in range(bits):
        absorb(last, stage)
        if stage + 1 < bits:
            launch(last, stage + 1)
        if stage < hops:
            spread(stage).wait_recv()
            if stage + 1 < hops:
                spread(stage + 1).start()
    for hop in range(bits, hops):
        spread(hop).wait_recv()
        if hop + 1 < hops:
            spread(hop + 1).start()
    for hop in range(hops):
        spread(hop).wait_send()
    for stage in range(bits):
        fly(stage).wait_send()

    @pl.loop(0, chunks)
    def _(q):
        for hop in range(hops):
            for piece in range(2):
                ring(q, hop, piece).wait_send()
        for side in range(2):
            for stage in range(bits):
                cut(q, side, stage).wait_send()


def normalize(counts, library):
    factor = 10000.0 / library.astype(jnp.float32)
    return jnp.log1p(counts.astype(jnp.float32) * factor[:, None]).astype(jnp.bfloat16)


def shards(counts, library):
    own_block = normalize(counts, library)
    cells, col_width = own_block.shape
    cell_groups = lax.axis_size("cells")
    gene_groups = lax.axis_size("genes")
    row_width = col_width * gene_groups // cell_groups
    owners = col_width // row_width
    total_cells = float(cells * cell_groups)
    me = lax.axis_index("genes")

    chunks = min(CHUNKS, row_width // 16)
    part = row_width // chunks
    ordered = own_block.T.reshape(owners, chunks, part, cells)
    widened = own_block.astype(jnp.float32)
    sums = jnp.stack([jnp.sum(widened, axis=0), jnp.sum(widened * widened, axis=0)])
    sums = jnp.concatenate([sums, jnp.zeros((6, col_width), jnp.float32)], axis=0)
    bits = cell_groups.bit_length() - 1
    hops = gene_groups - 1
    vmem = pl.BlockSpec(memory_space=pltpu.VMEM)
    dma = pltpu.SemaphoreType.DMA
    gram_tile, stats = pl.pallas_call(
        functools.partial(network, cell_groups, gene_groups),
        out_shape=(
            jax.ShapeDtypeStruct((row_width, col_width), jnp.float32),
            jax.ShapeDtypeStruct((gene_groups, 8, col_width), jnp.float32),
        ),
        in_specs=[vmem] * 3,
        out_specs=(vmem, vmem),
        scratch_shapes=[
            pltpu.VMEM((chunks, hops, owners, part, cells), jnp.bfloat16),
            pltpu.VMEM((chunks, 2, cell_groups, part, col_width // 2), jnp.float32),
            pltpu.VMEM((chunks, 2, cell_groups, part, col_width // 2), jnp.float32),
            pltpu.VMEM((bits + 1, 8, col_width), jnp.float32),
            pltpu.VMEM((bits, 8, col_width), jnp.float32),
            dma((chunks, hops, 2)), dma((chunks, hops, 2)),
            dma((chunks, 2, bits)), dma((chunks, 2, bits)),
            dma((bits,)), dma((bits,)),
            dma((hops,)), dma((hops,)),
        ],
        compiler_params=pltpu.CompilerParams(
            collective_id=0, has_side_effects=True, vmem_limit_bytes=60 * 1024 * 1024),
    )(ordered, own_block, sums)
    order = lax.rem(me - jnp.arange(gene_groups) + gene_groups, gene_groups)
    all_sums = jnp.transpose(jnp.take(stats[:, :2], order, axis=0), (1, 0, 2)).reshape(2, -1)

    means = all_sums[0] / total_cells
    variances = all_sums[1] / total_cells - means * means
    scales = lax.rsqrt(variances + 1e-05)
    row_first = lax.axis_index("cells") * row_width
    col_first = me * col_width
    row_means = lax.dynamic_slice_in_dim(means, row_first, row_width, 0)
    col_means = lax.dynamic_slice_in_dim(means, col_first, col_width, 0)
    row_scales = lax.dynamic_slice_in_dim(scales, row_first, row_width, 0)
    col_scales = lax.dynamic_slice_in_dim(scales, col_first, col_width, 0)
    correlation = (
        (gram_tile / total_cells - row_means[:, None] * col_means[None, :])
        * row_scales[:, None]
        * col_scales[None, :]
    )
    powered = correlation**6
    row_index = row_first + jnp.arange(row_width, dtype=jnp.int32)[:, None]
    col_index = col_first + jnp.arange(col_width, dtype=jnp.int32)[None, :]
    adjacency = jnp.where(row_index == col_index, jnp.float32(0.0), powered)
    connectivity = lax.psum(jnp.sum(adjacency, axis=1), "genes")
    return (adjacency, connectivity)


def solution(mesh):
    sized = mesh.shape["genes"] == 4 and mesh.shape["cells"] == 8

    def body(counts, library):
        cells, block = counts.shape
        if sized and cells % 1024 == 0 and block % 512 == 0:
            return by_planes(counts, library)
        return shards(counts, library)

    return jax.shard_map(
        body,
        mesh=mesh,
        in_specs=(P("cells", "genes"), P("cells")),
        out_specs=(P("cells", "genes"), P("cells")),
        check_vma=False,
    )
```

```python
import functools

import jax
import jax.numpy as jnp
from jax import lax
from jax.experimental import pallas as pl
from jax.experimental.pallas import tpu as pltpu
from jax.sharding import PartitionSpec as P

CHUNKS = 8
TILE = 512
QUARTERS = 4
UNIT = 28000.0
FOLDED = tuple(min(16, max(0, n - 1)) for n in range(20))
SUMMED = tuple(min(16, max(0, n - 3)) for n in range(20))
NEAR_ORDER = (0, 1, 2, 3, 4, 5, 6, 7, 8, 9, 10, 12, 11, 13, 14, 15)
GO_AT = 6
MESH = pl.DeviceIdType.MESH


def bit(value, index):
    return (value // (1 << index)) % 2


def flip(value, index):
    return value + (1 << index) * (1 - 2 * bit(value, index))


def planes(counts_ref, library_ref, out_ref, conn_ref,
           raw, own, sums_ref, squares, result, sib, stat, held, stream, tiles, land1, land2, whole, outn, outt, inbox,
           pstat, message, table, columns, lanes, cmsg, cin,
           stat_send, stat_recv, held_send, held_recv, sib_send, sib_recv, stream_send, stream_recv, pass_send, onward_send, go,
           one_send, one_recv, two_send, two_recv, hand_send, hand_recv, norm_send, turn_send, in_recv,
           load_done, store_done, sum_send, sum_recv, row_send, row_recv, conn_send, conn_recv):
    quarters, width, cells = own.shape
    total_cells = float(cells * 8)
    c = lax.axis_index("cells")
    g = lax.axis_index("genes")
    chip = c // 2
    core = c % 2
    side = g // 2
    far = 3 * side
    near = 1 + side
    beyond = 2 - side
    farther = 3 - 3 * side
    other = c + 1 - 2 * core
    inner = (g == 1) | (g == 2)
    outer = (g == 0) | (g == 3)
    lead = core == side
    aux = core != side

    barrier = pltpu.get_barrier_semaphore()

    @pl.loop(1, 32)
    def _(d):
        t = lax.rem(c * 4 + g + d, 32)
        pl.semaphore_signal(barrier, inc=1, device_id=(t // 4, lax.rem(t, 4)), device_id_type=MESH)

    slabs, slab, block = raw.shape

    def load(r):
        return pltpu.make_async_copy(counts_ref.at[pl.ds(r * slab, slab)], raw.at[r], load_done.at[r])

    @pl.loop(0, slabs)
    def _(r):
        load(r).start()

    sums_ref[...] = jnp.zeros_like(sums_ref)
    squares[...] = jnp.zeros_like(squares)

    @pl.loop(0, slabs)
    def _(r):
        load(r).wait()
        factor = 10000.0 / library_ref[pl.ds(r, 1), :].astype(jnp.float32)
        factor = jnp.transpose(jnp.broadcast_to(factor, (8, slab)))[:, 0:1]
        expressed = jnp.log1p(raw[r].astype(jnp.float32) * factor).astype(jnp.bfloat16).astype(jnp.float32)
        sums_ref[...] = sums_ref[...] + jnp.sum(expressed.reshape(slab // 8, 8, block), axis=0)
        squares[...] = squares[...] + jnp.sum((expressed * expressed).reshape(slab // 8, 8, block), axis=0)
        turned_slab = jnp.transpose(expressed).astype(jnp.bfloat16).reshape(quarters, width, slab)
        own[:, :, pl.ds(pl.multiple_of(r * slab, slab), slab)] = turned_slab

    total_sum = jnp.sum(sums_ref[...], axis=0, keepdims=True)
    total_square = jnp.sum(squares[...], axis=0, keepdims=True)
    sums_ref[...] = jnp.zeros_like(sums_ref)
    sums_ref[0:1] = total_sum
    sums_ref[1:2] = total_square

    def remote(src, dst, send, recv, device):
        return pltpu.make_async_remote_copy(
            src_ref=src, dst_ref=dst, send_sem=send, recv_sem=recv, device_id=device, device_id_type=MESH)

    def share():
        return remote(own, sib, sib_send, sib_recv, (other, g))

    def across(q):
        return remote(own.at[q], stream.at[q], stream_send.at[q], stream_recv.at[q], (other, beyond))

    def inward(q):
        return remote(own.at[q], held.at[q], stream_send.at[q], held_recv.at[q], (c, near))

    def relay(q):
        return remote(held.at[q], stream.at[4 + q], stream_send.at[4 + q], stream_recv.at[4 + q], (other, beyond))

    def beside(q):
        return remote(held.at[q], held.at[q], held_send.at[q], held_recv.at[q], (other, g))

    def passed(t):
        return remote(stream.at[t], stream.at[t], pass_send.at[t], stream_recv.at[t], (other, g))

    def onward(t):
        return remote(stream.at[t], stream.at[t], onward_send.at[t], stream_recv.at[t], (other, far))

    def swap(q):
        return remote(own.at[q], stat.at[q], stat_send.at[q], stat_recv.at[q], (c, near))

    def local_sums(d):
        return remote(sums_ref, pstat.at[c], sum_send.at[d], sum_recv.at[c], (lax.rem(c + d, 8), g))

    def sums_from(d):
        source = lax.rem(c + d, 8)
        return remote(sums_ref, pstat.at[source], sum_send.at[d], sum_recv.at[source], (source, g))

    def genes_to(d):
        return remote(message, table.at[g], row_send.at[d], row_recv.at[g], (c, lax.rem(g + d, 4)))

    def genes_from(d):
        source = lax.rem(g + d, 4)
        return remote(message, table.at[source], row_send.at[d], row_recv.at[source], (c, source))

    def conn_to(d):
        return remote(cmsg, cin.at[g], conn_send.at[d], conn_recv.at[g], (c, lax.rem(g + d, 4)))

    def conn_from(d):
        source = lax.rem(g + d, 4)
        return remote(cmsg, cin.at[source], conn_send.at[d], conn_recv.at[source], (c, source))

    crossing = chip // 2 != side

    @pl.when(chip // 2 == side)
    def _():
        inbox[1 - side] = jnp.zeros(inbox.shape[1:], inbox.dtype)

    pl.semaphore_wait(barrier, 31)

    for d in range(1, 8):
        local_sums(d).start()

    @pl.when(aux & inner)
    def _():
        across(0).start()

    @pl.when(aux & outer)
    def _():
        inward(0).start()

    @pl.when(aux)
    def _():
        share().start()

    pstat[c] = sums_ref[...]
    for d in range(1, 8):
        sums_from(d).wait_recv()
    everyone = pstat[0]
    for d in range(1, 8):
        everyone = everyone + pstat[d]
    together = pstat[2 * chip] + pstat[2 * chip + 1]
    means = everyone[0:1] / total_cells
    variances = everyone[1:2] / total_cells - means * means
    scales = lax.rsqrt(variances + 1e-05)
    message[0:1] = means
    message[1:2] = scales * ((UNIT / total_cells) ** 0.5)
    message[2:3] = sums_ref[0:1]
    message[3:4] = together[0:1]
    message[4:8] = jnp.zeros((4, block), jnp.float32)
    table[g] = message[...]
    for d in range(1, 4):
        genes_to(d).start()

    @pl.when(aux & inner)
    def _():
        for q in range(1, 4):
            across(q).start()
        for q in range(4):
            inward(q).wait_recv()
            relay(q).start()
            beside(q).start()
            across(q).wait_recv()
            passed(q).start()
            onward(q).start()
        for q in range(4):
            relay(q).wait_recv()
            passed(4 + q).start()
            onward(4 + q).start()

    @pl.when(aux & outer)
    def _():
        for q in range(1, 4):
            inward(q).start()
        for q in range(4):
            inward(q).wait_send()
        pl.semaphore_signal(go, inc=1, device_id=(other, g), device_id_type=MESH)

    @pl.when(aux)
    def _():
        for d in range(1, 4):
            genes_from(d).wait_recv()

    def where(test, yes, no):
        return jnp.where(test, yes, no)

    def first_axis(idx):
        return 1 + 0 * idx

    def turn(value, step):
        return value + step * (1 - 2 * ((value // step) % 2))

    def place(piece, idx):
        one = first_axis(idx)
        two = 3 - one
        return (2 * ((piece // one + chip // one) % 2) + (piece // two + chip // two) % 2)

    def fold_one(idx):
        partner = turn(chip, first_axis(idx))
        return remote(tiles.at[idx, pl.ds(2, 2)], land1.at[idx], one_send.at[idx], one_recv.at[idx],
                      (2 * partner + core, g))

    def fold_two(idx):
        partner = turn(chip, 3 - first_axis(idx))
        return remote(tiles.at[idx, 1], land2.at[idx], two_send.at[idx], two_recv.at[idx],
                      (2 * partner + core, g))

    def task_at(n):
        code = 0
        for index, near_task in enumerate(NEAR_ORDER):
            code = where(n == index, where(inner, near_task, index), code)
        return code

    def reached(table, n):
        value = 0
        for index, entry in enumerate(table):
            value = where(n == index, entry, value)
        return jnp.minimum(value, tasks)

    tasks = where(inner, 16, 12)

    def rows_of(idx):
        crossed = where(idx < 8, beyond, where(idx < 12, farther, far))
        return where(idx < 4, g, crossed)

    def hand(idx):
        return remote(whole.at[idx], outn.at[idx], hand_send.at[idx], hand_recv.at[idx], (other, g))

    def normal(idx):
        q = idx % 4
        return remote(whole.at[idx], inbox.at[side, q % 2, chip], norm_send.at[idx], in_recv.at[side, q % 2, chip],
                      (2 * rows_of(idx) + q // 2, g))

    def turned(idx):
        q = idx % 4
        return remote(outt.at[idx], inbox.at[side, chip % 2, q], turn_send.at[idx], in_recv.at[side, chip % 2, q],
                      (2 * g + chip // 2, rows_of(idx)))

    def normal_here(idx):
        return 2 * rows_of(idx) + (idx % 4) // 2 == c

    def absorb_one(idx):
        fold_one(idx).wait_recv()
        tiles[idx, 1] = (tiles[idx, 1].astype(jnp.int32) + land1[idx, 1].astype(jnp.int32)).astype(jnp.int16)
        fold_two(idx).start()

    def absorb_two(idx):
        fold_two(idx).wait_recv()
        total = (tiles[idx, 0].astype(jnp.int32) + land1[idx, 0].astype(jnp.int32)
                 + land2[idx].astype(jnp.int32))
        whole[idx] = total.astype(jnp.int16)

        @pl.when(idx >= 4)
        def _():
            hand(idx).start()
        here = normal_here(idx)

        @pl.when(here)
        def _():
            inbox[side, (idx % 4) % 2, chip] = total.astype(jnp.int16)

        @pl.when(jnp.logical_not(here))
        def _():
            normal(idx).start()

    def deliver(idx):
        hand(idx).wait_recv()
        outt[idx] = jnp.transpose(outn[idx].astype(jnp.int32)).astype(jnp.int16)
        turned(idx).start()

    def product(idx, row, count, parts):
        row_block = rows_of(idx)
        col_block = g
        first = pl.multiple_of((idx % 4) * width, width)
        stats = columns[row_block, pl.ds(first, width), :]
        scale_j = stats[:, 1:2]
        mean_j = scale_j * stats[:, 0:1]
        sum_j = scale_j * stats[:, row:row + 1]

        @pl.loop(0, quarters)
        def _(p):
            acc = 0.0
            for left, right in parts:
                acc = acc + lax.dot_general(left[...], right(p)[...], (((1,), (1,)), ((), ())),
                                            preferred_element_type=jnp.float32)
            span = pl.ds(pl.multiple_of(p * width, width), width)
            mean_i = table[col_block, 0:1, span]
            scale_i = table[col_block, 1:2, span]
            drift_i = table[col_block, row:row + 1, span] - count * mean_i
            value = (acc * scale_j - mean_j * drift_i - sum_j * mean_i) * scale_i
            tiles[idx, place(p, idx)] = jnp.round(value).astype(jnp.int32).astype(jnp.int16)

    def step(idx):
        q = idx % 4

        @pl.when(idx == 4)
        def _():
            for d in range(1, 4):
                genes_from(d).wait_recv()
                z = lax.rem(g + d, 4)
                columns[z] = jnp.transpose(table[z])

        @pl.when(outer & (idx == GO_AT))
        def _():
            pl.semaphore_wait(go, 1)
            for t in range(4):
                swap(t).start()

        @pl.when(idx < 4)
        def _():
            product(idx, 3, 2.0 * cells,
                    [(own.at[q], lambda p: own.at[p]), (sib.at[q], lambda p: sib.at[p])])

        @pl.when((idx >= 4) & (idx < 12))
        def _():
            slot = idx - 4
            passed(slot).wait_recv()
            product(idx, 2, 1.0 * cells, [(stream.at[slot], lambda p: own.at[p])])

        @pl.when(idx >= 12)
        def _():
            swap(q).wait_recv()
            beside(q).wait_recv()
            product(idx, 3, 2.0 * cells,
                    [(stat.at[q], lambda p: own.at[p]), (held.at[q], lambda p: sib.at[p])])

        fold_one(idx).start()

    @pl.when(lead)
    def _():
        columns[g] = jnp.transpose(table[g])
        share().wait_recv()

        @pl.loop(0, len(FOLDED))
        def _(n):
            @pl.when(n < tasks)
            def _():
                step(task_at(n))

            @pl.loop(reached(FOLDED, n - 1), reached(FOLDED, n))
            def _(m):
                absorb_one(task_at(m))

            @pl.loop(reached(SUMMED, n - 1), reached(SUMMED, n))
            def _(m):
                absorb_two(task_at(m))

    @pl.when(aux)
    def _():
        @pl.loop(4, tasks)
        def _(n):
            deliver(task_at(n))

    def store(r, piece):
        down = pl.ds(pl.multiple_of(r * width, width), width)
        along = pl.ds(pl.multiple_of(piece * width, width), width)
        return pltpu.make_async_copy(result.at[r, piece], out_ref.at[down, along], store_done.at[r, piece])

    lanes[...] = jnp.zeros_like(lanes)
    height = 2 * width

    @pl.loop(0, 8)
    def _(n):
        piece = n // 2
        r = n % 2
        mine = (chip == piece) & (crossing | (chip == g) | inner)

        @pl.when(jnp.logical_not(mine & lead))
        def _():
            remote(outn.at[0], inbox.at[side, r, piece], norm_send.at[0], in_recv.at[side, r, piece],
                   (other, g)).wait_recv()

        @pl.when(crossing)
        def _():
            remote(outn.at[0], inbox.at[1 - side, r, piece], norm_send.at[0], in_recv.at[1 - side, r, piece],
                   (other, g)).wait_recv()
        total = inbox[0, r, piece].astype(jnp.int32) + inbox[1, r, piece].astype(jnp.int32)
        result[r, piece] = total.astype(jnp.int16)
        store(r, piece).start()
        value = total.astype(jnp.float32) * (1.0 / UNIT)
        square = value * value
        powered = square * square * square
        rows = c * height + r * width + lax.broadcasted_iota(jnp.int32, (width, width), 0)
        cols = g * block + piece * width + lax.broadcasted_iota(jnp.int32, (width, width), 1)
        powered = jnp.where(rows == cols, 0.0, powered)
        down = pl.ds(pl.multiple_of(r * width, width), width)
        part = powered[:, 0:128]
        for lane in range(1, width // 128):
            part = part + powered[:, lane * 128:(lane + 1) * 128]
        lanes[down, :] = lanes[down, :] + part

    cmsg[...] = jnp.broadcast_to(jnp.sum(jnp.transpose(lanes[...]), axis=0, keepdims=True), cmsg.shape)
    for d in range(1, 4):
        conn_to(d).start()
    for d in range(1, 8):
        local_sums(d).wait_send()
    for d in range(1, 4):
        genes_to(d).wait_send()

    @pl.when(aux)
    def _():
        share().wait_send()

    @pl.when(aux & inner)
    def _():
        for q in range(4):
            across(q).wait_send()
            relay(q).wait_send()
            beside(q).wait_send()
        for t in range(8):
            passed(t).wait_send()
            onward(t).wait_send()

    @pl.when(lead & outer)
    def _():
        for q in range(4):
            swap(q).wait_send()

    @pl.when(lead)
    def _():
        @pl.loop(0, tasks)
        def _(idx):
            fold_one(idx).wait_send()
            fold_two(idx).wait_send()

            @pl.when(idx >= 4)
            def _():
                hand(idx).wait_send()

            @pl.when(jnp.logical_not(normal_here(idx)))
            def _():
                normal(idx).wait_send()

    @pl.when(aux)
    def _():
        @pl.loop(4, tasks)
        def _(idx):
            turned(idx).wait_send()

    cin[g] = cmsg[...]
    for d in range(1, 4):
        conn_from(d).wait_recv()
    conn_ref[...] = ((cin[0] + cin[1]) + (cin[2] + cin[3]))[0:1]

    @pl.loop(0, 8)
    def _(n):
        store(n % 2, n // 2).wait()
    for d in range(1, 4):
        conn_to(d).wait_send()


def by_planes(counts, library):
    cells, block = counts.shape
    width = block // QUARTERS
    slab = 128
    vmem = pl.BlockSpec(memory_space=pltpu.VMEM)
    anywhere = pl.BlockSpec(memory_space=pl.ANY)
    dma = pltpu.SemaphoreType.DMA
    small = jnp.int16
    count = 16
    quarters = pltpu.VMEM((QUARTERS, width, cells), jnp.bfloat16)
    pieces = pltpu.VMEM((count, width, width), small)
    row = pltpu.VMEM((8, block), jnp.float32)
    totals, connectivity = pl.pallas_call(
        planes,
        out_shape=(
            jax.ShapeDtypeStruct((2 * width, block), small),
            jax.ShapeDtypeStruct((1, 2 * width), jnp.float32),
        ),
        in_specs=[anywhere, vmem],
        out_specs=(anywhere, vmem),
        scratch_shapes=[
            pltpu.VMEM((cells // slab, slab, block), jnp.int32),
            quarters, row, row,
            pltpu.VMEM((2, 4, width, width), small),
            quarters, quarters, quarters,
            pltpu.VMEM((8, width, cells), jnp.bfloat16),
            pltpu.VMEM((count, 4, width, width), small),
            pltpu.VMEM((count, 2, width, width), small),
            pieces, pieces, pieces, pieces,
            pltpu.VMEM((2, 2, 4, width, width), small),
            pltpu.VMEM((8, 8, block), jnp.float32),
            row,
            pltpu.VMEM((4, 8, block), jnp.float32),
            pltpu.VMEM((4, block, 8), jnp.float32),
            pltpu.VMEM((2 * width, 128), jnp.float32),
            pltpu.VMEM((8, 2 * width), jnp.float32),
            pltpu.VMEM((4, 8, 2 * width), jnp.float32),
            dma((4,)), dma((4,)), dma((4,)), dma((4,)), dma, dma, dma((8,)), dma((8,)), dma((8,)), dma((8,)), pltpu.SemaphoreType.REGULAR,
            dma((count,)), dma((count,)), dma((count,)), dma((count,)), dma((count,)), dma((count,)),
            dma((count,)), dma((count,)), dma((2, 2, 4)),
            dma((cells // slab,)), dma((2, 4)),
            dma((8,)), dma((8,)), dma((4,)), dma((4,)), dma((4,)), dma((4,)),
        ],
        compiler_params=pltpu.CompilerParams(
            collective_id=1, has_side_effects=True, vmem_limit_bytes=58 * 1024 * 1024),
    )(counts, library.reshape(cells // slab, slab))
    value = totals.astype(jnp.float32) * (1.0 / UNIT)
    square = value * value
    rows = lax.axis_index("cells") * 2 * width + jnp.arange(2 * width, dtype=jnp.int32)[:, None]
    cols = lax.axis_index("genes") * block + jnp.arange(block, dtype=jnp.int32)[None, :]
    adjacency = jnp.where(rows == cols, jnp.float32(0.0), square * square * square)
    return adjacency, connectivity.reshape(2 * width)


def network(cell_groups, gene_groups, xq_ref, own_ref, sums_ref, out_ref, stats_ref,
            held, partial, landed, totals, sums_in,
            ring_send, ring_recv, cut_send, cut_recv, fly_send, fly_recv, stat_send, stat_recv):
    owners, chunks, part, cells = xq_ref.shape
    rows = owners * part
    cols = own_ref.shape[1]
    half = cols // 2
    c = lax.axis_index("cells")
    g = lax.axis_index("genes")
    right = lax.rem(g + 1, gene_groups)
    left = lax.rem(g + gene_groups - 1, gene_groups)
    bits = cell_groups.bit_length() - 1
    hops = gene_groups - 1
    orders = (tuple(range(bits)), (0,) + tuple(range(bits - 1, 0, -1)))

    barrier = pltpu.get_barrier_semaphore()
    for target in [(c, left), (c, right)] + [(flip(c, b), g) for b in range(bits)]:
        pl.semaphore_signal(barrier, inc=1, device_id=target, device_id_type=pl.DeviceIdType.MESH)
    pl.semaphore_wait(barrier, 2 + bits)

    def ring(q, hop, piece):
        span = pl.ds(piece * (owners // 2), owners // 2)
        source = xq_ref.at[span, q] if hop == 0 else held.at[q, hop - 1, span]
        return pltpu.make_async_remote_copy(
            src_ref=source, dst_ref=held.at[q, hop, span],
            send_sem=ring_send.at[q, hop, piece], recv_sem=ring_recv.at[q, hop, piece],
            device_id=(c, right), device_id_type=pl.DeviceIdType.MESH)

    def cut(q, side, stage):
        count = cell_groups >> (stage + 1)
        return pltpu.make_async_remote_copy(
            src_ref=partial.at[q, side, pl.ds(count, count)],
            dst_ref=landed.at[q, side, pl.ds(count, count)],
            send_sem=cut_send.at[q, side, stage], recv_sem=cut_recv.at[q, side, stage],
            device_id=(flip(c, orders[side][stage]), g), device_id_type=pl.DeviceIdType.MESH)

    def fly(stage):
        return pltpu.make_async_remote_copy(
            src_ref=totals.at[stage], dst_ref=sums_in.at[stage],
            send_sem=fly_send.at[stage], recv_sem=fly_recv.at[stage],
            device_id=(flip(c, stage), g), device_id_type=pl.DeviceIdType.MESH)

    def spread(hop):
        source = totals.at[bits] if hop == 0 else stats_ref.at[hop]
        return pltpu.make_async_remote_copy(
            src_ref=source, dst_ref=stats_ref.at[hop + 1],
            send_sem=stat_send.at[hop], recv_sem=stat_recv.at[hop],
            device_id=(c, right), device_id_type=pl.DeviceIdType.MESH)

    def place(owner, side):
        total = 0
        for position, b in enumerate(orders[side]):
            total = total + ((bit(owner, b) + bit(c, b)) % 2) * (1 << (bits - 1 - position))
        return total

    def multiply(q, step):
        source = lax.rem(g - step + gene_groups, gene_groups)
        block = xq_ref.at[:, q] if step == 0 else held.at[q, step - 1]
        for side in range(2):
            spots = [place(source * owners + o, side) for o in range(owners)]

            @pl.loop(0, half // TILE)
            def _(t):
                start = pl.multiple_of(t * TILE, TILE)
                columns = pl.ds(pl.multiple_of(side * half + start, TILE), TILE)
                tile = jnp.dot(block[...].reshape(rows, cells), own_ref[:, columns], preferred_element_type=jnp.float32)
                for o in range(owners):
                    partial[q, side, spots[o], :, pl.ds(start, TILE)] = tile[o * part:(o + 1) * part]

    def launch(q, stage):
        for side in range(2):
            cut(q, side, stage).start()

    def absorb(q, stage):
        count = cell_groups >> (stage + 1)
        for side in range(2):
            cut(q, side, stage).wait_recv()
            if count > 1:
                @pl.loop(0, count)
                def _(i):
                    partial[q, side, i] = partial[q, side, i] + landed[q, side, i + count]
            else:
                out_ref[pl.ds(q * part, part), side * half:(side + 1) * half] = (
                    partial[q, side, 0] + landed[q, side, 1])

    for piece in range(2):
        ring(0, 0, piece).start()
    totals[0] = sums_ref[...]
    for stage in range(bits):
        fly(stage).start()
        fly(stage).wait_recv()
        totals[stage + 1] = totals[stage] + sums_in[stage]
    stats_ref[0] = totals[bits]

    turns = [[s for s in range(bits) if s * hops // bits == h] for h in range(hops)]

    @pl.loop(0, chunks)
    def _(q):
        multiply(q, 0)
        for hop in range(hops):
            for piece in range(2):
                ring(q, hop, piece).wait_recv()
                if hop < hops - 1:
                    ring(q, hop + 1, piece).start()
            if hop == max(hops - 2, 0):
                @pl.when(q < chunks - 1)
                def _():
                    for piece in range(2):
                        ring(q + 1, 0, piece).start()

            @pl.when(q > 0)
            def _():
                for stage in turns[hop]:
                    absorb(q - 1, stage)
                    if stage + 1 < bits:
                        launch(q - 1, stage + 1)
            multiply(q, hop + 1)
        launch(q, 0)

    last = chunks - 1
    spread(0).start()
    for stage in range(bits):
        absorb(last, stage)
        if stage + 1 < bits:
            launch(last, stage + 1)
        if stage < hops:
            spread(stage).wait_recv()
            if stage + 1 < hops:
                spread(stage + 1).start()
    for hop in range(bits, hops):
        spread(hop).wait_recv()
        if hop + 1 < hops:
            spread(hop + 1).start()
    for hop in range(hops):
        spread(hop).wait_send()
    for stage in range(bits):
        fly(stage).wait_send()

    @pl.loop(0, chunks)
    def _(q):
        for hop in range(hops):
            for piece in range(2):
                ring(q, hop, piece).wait_send()
        for side in range(2):
            for stage in range(bits):
                cut(q, side, stage).wait_send()


def normalize(counts, library):
    factor = 10000.0 / library.astype(jnp.float32)
    return jnp.log1p(counts.astype(jnp.float32) * factor[:, None]).astype(jnp.bfloat16)


def shards(counts, library):
    own_block = normalize(counts, library)
    cells, col_width = own_block.shape
    cell_groups = lax.axis_size("cells")
    gene_groups = lax.axis_size("genes")
    row_width = col_width * gene_groups // cell_groups
    owners = col_width // row_width
    total_cells = float(cells * cell_groups)
    me = lax.axis_index("genes")

    chunks = min(CHUNKS, row_width // 16)
    part = row_width // chunks
    ordered = own_block.T.reshape(owners, chunks, part, cells)
    widened = own_block.astype(jnp.float32)
    sums = jnp.stack([jnp.sum(widened, axis=0), jnp.sum(widened * widened, axis=0)])
    sums = jnp.concatenate([sums, jnp.zeros((6, col_width), jnp.float32)], axis=0)
    bits = cell_groups.bit_length() - 1
    hops = gene_groups - 1
    vmem = pl.BlockSpec(memory_space=pltpu.VMEM)
    dma = pltpu.SemaphoreType.DMA
    gram_tile, stats = pl.pallas_call(
        functools.partial(network, cell_groups, gene_groups),
        out_shape=(
            jax.ShapeDtypeStruct((row_width, col_width), jnp.float32),
            jax.ShapeDtypeStruct((gene_groups, 8, col_width), jnp.float32),
        ),
        in_specs=[vmem] * 3,
        out_specs=(vmem, vmem),
        scratch_shapes=[
            pltpu.VMEM((chunks, hops, owners, part, cells), jnp.bfloat16),
            pltpu.VMEM((chunks, 2, cell_groups, part, col_width // 2), jnp.float32),
            pltpu.VMEM((chunks, 2, cell_groups, part, col_width // 2), jnp.float32),
            pltpu.VMEM((bits + 1, 8, col_width), jnp.float32),
            pltpu.VMEM((bits, 8, col_width), jnp.float32),
            dma((chunks, hops, 2)), dma((chunks, hops, 2)),
            dma((chunks, 2, bits)), dma((chunks, 2, bits)),
            dma((bits,)), dma((bits,)),
            dma((hops,)), dma((hops,)),
        ],
        compiler_params=pltpu.CompilerParams(
            collective_id=0, has_side_effects=True, vmem_limit_bytes=60 * 1024 * 1024),
    )(ordered, own_block, sums)
    order = lax.rem(me - jnp.arange(gene_groups) + gene_groups, gene_groups)
    all_sums = jnp.transpose(jnp.take(stats[:, :2], order, axis=0), (1, 0, 2)).reshape(2, -1)

    means = all_sums[0] / total_cells
    variances = all_sums[1] / total_cells - means * means
    scales = lax.rsqrt(variances + 1e-05)
    row_first = lax.axis_index("cells") * row_width
    col_first = me * col_width
    row_means = lax.dynamic_slice_in_dim(means, row_first, row_width, 0)
    col_means = lax.dynamic_slice_in_dim(means, col_first, col_width, 0)
    row_scales = lax.dynamic_slice_in_dim(scales, row_first, row_width, 0)
    col_scales = lax.dynamic_slice_in_dim(scales, col_first, col_width, 0)
    correlation = (
        (gram_tile / total_cells - row_means[:, None] * col_means[None, :])
        * row_scales[:, None]
        * col_scales[None, :]
    )
    powered = correlation**6
    row_index = row_first + jnp.arange(row_width, dtype=jnp.int32)[:, None]
    col_index = col_first + jnp.arange(col_width, dtype=jnp.int32)[None, :]
    adjacency = jnp.where(row_index == col_index, jnp.float32(0.0), powered)
    connectivity = lax.psum(jnp.sum(adjacency, axis=1), "genes")
    return (adjacency, connectivity)


def solution(mesh):
    sized = mesh.shape["genes"] == 4 and mesh.shape["cells"] == 8

    def body(counts, library):
        cells, block = counts.shape
        if sized and cells % 1024 == 0 and block % 512 == 0:
            return by_planes(counts, library)
        return shards(counts, library)

    return jax.shard_map(
        body,
        mesh=mesh,
        in_specs=(P("cells", "genes"), P("cells")),
        out_specs=(P("cells", "genes"), P("cells")),
        check_vma=False,
    )
```

```python
import functools

import jax
import jax.numpy as jnp
from jax import lax
from jax.experimental import pallas as pl
from jax.experimental.pallas import tpu as pltpu
from jax.sharding import PartitionSpec as P

CHUNKS = 8
TILE = 512
QUARTERS = 4
UNIT = 28000.0
FOLDED = tuple(min(16, max(0, n - 1)) for n in range(20))
SUMMED = tuple(min(16, max(0, n - 3)) for n in range(20))
NEAR_ORDER = (0, 1, 2, 3, 4, 5, 6, 7, 8, 9, 10, 12, 11, 13, 14, 15)
GO_AT = 6
MESH = pl.DeviceIdType.MESH


def bit(value, index):
    return (value // (1 << index)) % 2


def flip(value, index):
    return value + (1 << index) * (1 - 2 * bit(value, index))


def planes(counts_ref, library_ref, out_ref, conn_ref,
           raw, own, sums_ref, squares, result, sib, stat, held, stream, tiles, land1, land2, whole, outn, outt, inbox,
           pstat, message, table, columns, lanes, cmsg, cin,
           stat_send, stat_recv, held_send, held_recv, sib_send, sib_recv, stream_send, stream_recv, pass_send, onward_send, go,
           one_send, one_recv, two_send, two_recv, hand_send, hand_recv, norm_send, turn_send, in_recv,
           load_done, store_done, sum_send, sum_recv, row_send, row_recv, conn_send, conn_recv):
    quarters, width, cells = own.shape
    total_cells = float(cells * 8)
    c = lax.axis_index("cells")
    g = lax.axis_index("genes")
    chip = c // 2
    core = c % 2
    side = g // 2
    far = 3 * side
    near = 1 + side
    beyond = 2 - side
    farther = 3 - 3 * side
    other = c + 1 - 2 * core
    inner = (g == 1) | (g == 2)
    outer = (g == 0) | (g == 3)
    lead = core == side
    aux = core != side

    barrier = pltpu.get_barrier_semaphore()

    @pl.loop(1, 32)
    def _(d):
        t = lax.rem(c * 4 + g + d, 32)
        pl.semaphore_signal(barrier, inc=1, device_id=(t // 4, lax.rem(t, 4)), device_id_type=MESH)

    slabs, slab, block = raw.shape

    def load(r):
        return pltpu.make_async_copy(counts_ref.at[pl.ds(r * slab, slab)], raw.at[r], load_done.at[r])

    @pl.loop(0, slabs)
    def _(r):
        load(r).start()

    sums_ref[...] = jnp.zeros_like(sums_ref)
    squares[...] = jnp.zeros_like(squares)

    @pl.loop(0, slabs)
    def _(r):
        load(r).wait()
        factor = 10000.0 / library_ref[pl.ds(r, 1), :].astype(jnp.float32)
        factor = jnp.transpose(jnp.broadcast_to(factor, (8, slab)))[:, 0:1]
        expressed = jnp.log1p(raw[r].astype(jnp.float32) * factor).astype(jnp.bfloat16).astype(jnp.float32)
        sums_ref[...] = sums_ref[...] + jnp.sum(expressed.reshape(slab // 8, 8, block), axis=0)
        squares[...] = squares[...] + jnp.sum((expressed * expressed).reshape(slab // 8, 8, block), axis=0)
        turned_slab = jnp.transpose(expressed).astype(jnp.bfloat16).reshape(quarters, width, slab)
        own[:, :, pl.ds(pl.multiple_of(r * slab, slab), slab)] = turned_slab

    total_sum = jnp.sum(sums_ref[...], axis=0, keepdims=True)
    total_square = jnp.sum(squares[...], axis=0, keepdims=True)
    sums_ref[...] = jnp.zeros_like(sums_ref)
    sums_ref[0:1] = total_sum
    sums_ref[1:2] = total_square

    def remote(src, dst, send, recv, device):
        return pltpu.make_async_remote_copy(
            src_ref=src, dst_ref=dst, send_sem=send, recv_sem=recv, device_id=device, device_id_type=MESH)

    def share():
        return remote(own, sib, sib_send, sib_recv, (other, g))

    def across(q):
        return remote(own.at[q], stream.at[q], stream_send.at[q], stream_recv.at[q], (other, beyond))

    def inward(q):
        return remote(own.at[q], held.at[q], stream_send.at[q], held_recv.at[q], (c, near))

    def relay(q):
        return remote(held.at[q], stream.at[4 + q], stream_send.at[4 + q], stream_recv.at[4 + q], (other, beyond))

    def beside(q):
        return remote(held.at[q], held.at[q], held_send.at[q], held_recv.at[q], (other, g))

    def passed(t):
        return remote(stream.at[t], stream.at[t], pass_send.at[t], stream_recv.at[t], (other, g))

    def onward(t):
        return remote(stream.at[t], stream.at[t], onward_send.at[t], stream_recv.at[t], (other, far))

    def swap(q):
        return remote(own.at[q], stat.at[q], stat_send.at[q], stat_recv.at[q], (c, near))

    def local_sums(d):
        return remote(sums_ref, pstat.at[c], sum_send.at[d], sum_recv.at[c], (lax.rem(c + d, 8), g))

    def sums_from(d):
        source = lax.rem(c + d, 8)
        return remote(sums_ref, pstat.at[source], sum_send.at[d], sum_recv.at[source], (source, g))

    def genes_to(z):
        return remote(message, table.at[g], row_send.at[z], row_recv.at[g], (c, z))

    def genes_from(z):
        return remote(message, table.at[z], row_send.at[z], row_recv.at[z], (c, z))

    def conn_to(d):
        return remote(cmsg, cin.at[g], conn_send.at[d], conn_recv.at[g], (c, lax.rem(g + d, 4)))

    def conn_from(d):
        source = lax.rem(g + d, 4)
        return remote(cmsg, cin.at[source], conn_send.at[d], conn_recv.at[source], (c, source))

    crossing = chip // 2 != side

    @pl.when(chip // 2 == side)
    def _():
        inbox[1 - side] = jnp.zeros(inbox.shape[1:], inbox.dtype)

    pl.semaphore_wait(barrier, 31)

    for d in range(1, 8):
        local_sums(d).start()

    @pl.when(aux & inner)
    def _():
        across(0).start()

    @pl.when(aux & outer)
    def _():
        inward(0).start()

    @pl.when(aux)
    def _():
        share().start()

    pstat[c] = sums_ref[...]
    for d in range(1, 8):
        sums_from(d).wait_recv()
    everyone = pstat[0]
    for d in range(1, 8):
        everyone = everyone + pstat[d]
    together = pstat[2 * chip] + pstat[2 * chip + 1]
    means = everyone[0:1] / total_cells
    variances = everyone[1:2] / total_cells - means * means
    scales = lax.rsqrt(variances + 1e-05)
    message[0:1] = means
    message[1:2] = scales * ((UNIT / total_cells) ** 0.5)
    message[2:3] = sums_ref[0:1]
    message[3:4] = together[0:1]
    message[4:8] = jnp.zeros((4, block), jnp.float32)
    table[g] = message[...]
    pair = g + 1 - 2 * (g % 2)

    @pl.when(lead)
    def _():
        genes_to(pair).start()

    @pl.when(aux)
    def _():
        genes_to(beyond).start()
        genes_to(farther).start()

    @pl.when(aux & inner)
    def _():
        for q in range(1, 4):
            across(q).start()
        for q in range(4):
            inward(q).wait_recv()
            relay(q).start()
            beside(q).start()
            across(q).wait_recv()
            passed(q).start()
            onward(q).start()
        for q in range(4):
            relay(q).wait_recv()
            passed(4 + q).start()
            onward(4 + q).start()

    @pl.when(aux & outer)
    def _():
        for q in range(1, 4):
            inward(q).start()
        for q in range(4):
            inward(q).wait_send()
        pl.semaphore_signal(go, inc=1, device_id=(other, g), device_id_type=MESH)


    def where(test, yes, no):
        return jnp.where(test, yes, no)

    def first_axis(idx):
        return 1 + 0 * idx

    def turn(value, step):
        return value + step * (1 - 2 * ((value // step) % 2))

    def place(piece, idx):
        one = first_axis(idx)
        two = 3 - one
        return (2 * ((piece // one + chip // one) % 2) + (piece // two + chip // two) % 2)

    def fold_one(idx):
        partner = turn(chip, first_axis(idx))
        return remote(tiles.at[idx, pl.ds(2, 2)], land1.at[idx], one_send.at[idx], one_recv.at[idx],
                      (2 * partner + core, g))

    def fold_two(idx):
        partner = turn(chip, 3 - first_axis(idx))
        return remote(tiles.at[idx, 1], land2.at[idx], two_send.at[idx], two_recv.at[idx],
                      (2 * partner + core, g))

    def task_at(n):
        code = 0
        for index, near_task in enumerate(NEAR_ORDER):
            code = where(n == index, where(inner, near_task, index), code)
        return code

    def reached(table, n):
        value = 0
        for index, entry in enumerate(table):
            value = where(n == index, entry, value)
        return jnp.minimum(value, tasks)

    tasks = where(inner, 16, 12)

    def rows_of(idx):
        crossed = where(idx < 8, beyond, where(idx < 12, farther, far))
        return where(idx < 4, g, crossed)

    def hand(idx):
        return remote(whole.at[idx], outn.at[idx], hand_send.at[idx], hand_recv.at[idx], (other, g))

    def normal(idx):
        q = idx % 4
        return remote(whole.at[idx], inbox.at[side, q % 2, chip], norm_send.at[idx], in_recv.at[side, q % 2, chip],
                      (2 * rows_of(idx) + q // 2, g))

    def turned(idx):
        q = idx % 4
        return remote(outt.at[idx], inbox.at[side, chip % 2, q], turn_send.at[idx], in_recv.at[side, chip % 2, q],
                      (2 * g + chip // 2, rows_of(idx)))

    def normal_here(idx):
        return 2 * rows_of(idx) + (idx % 4) // 2 == c

    def absorb_one(idx):
        fold_one(idx).wait_recv()
        tiles[idx, 1] = (tiles[idx, 1].astype(jnp.int32) + land1[idx, 1].astype(jnp.int32)).astype(jnp.int16)
        fold_two(idx).start()

    def absorb_two(idx):
        fold_two(idx).wait_recv()
        total = (tiles[idx, 0].astype(jnp.int32) + land1[idx, 0].astype(jnp.int32)
                 + land2[idx].astype(jnp.int32))
        whole[idx] = total.astype(jnp.int16)

        @pl.when(idx >= 4)
        def _():
            hand(idx).start()
        here = normal_here(idx)

        @pl.when(here)
        def _():
            inbox[side, (idx % 4) % 2, chip] = total.astype(jnp.int16)

        @pl.when(jnp.logical_not(here))
        def _():
            normal(idx).start()

    def deliver(idx):
        hand(idx).wait_recv()
        outt[idx] = jnp.transpose(outn[idx].astype(jnp.int32)).astype(jnp.int16)
        turned(idx).start()

    def product(idx, row, count, parts):
        row_block = rows_of(idx)
        col_block = g
        first = pl.multiple_of((idx % 4) * width, width)
        stats = columns[row_block, pl.ds(first, width), :]
        scale_j = stats[:, 1:2]
        mean_j = scale_j * stats[:, 0:1]
        sum_j = scale_j * stats[:, row:row + 1]

        @pl.loop(0, quarters)
        def _(p):
            acc = 0.0
            for left, right in parts:
                acc = acc + lax.dot_general(left[...], right(p)[...], (((1,), (1,)), ((), ())),
                                            preferred_element_type=jnp.float32)
            span = pl.ds(pl.multiple_of(p * width, width), width)
            mean_i = table[col_block, 0:1, span]
            scale_i = table[col_block, 1:2, span]
            drift_i = table[col_block, row:row + 1, span] - count * mean_i
            value = (acc * scale_j - mean_j * drift_i - sum_j * mean_i) * scale_i
            tiles[idx, place(p, idx)] = jnp.round(value).astype(jnp.int32).astype(jnp.int16)

    def step(idx):
        q = idx % 4

        @pl.when(idx == 4)
        def _():
            for z in (pair, beyond, farther):
                genes_from(z).wait_recv()
                columns[z] = jnp.transpose(table[z])

        @pl.when(outer & (idx == GO_AT))
        def _():
            pl.semaphore_wait(go, 1)
            for t in range(4):
                swap(t).start()

        @pl.when(idx < 4)
        def _():
            product(idx, 3, 2.0 * cells,
                    [(own.at[q], lambda p: own.at[p]), (sib.at[q], lambda p: sib.at[p])])

        @pl.when((idx >= 4) & (idx < 12))
        def _():
            slot = idx - 4
            passed(slot).wait_recv()
            product(idx, 2, 1.0 * cells, [(stream.at[slot], lambda p: own.at[p])])

        @pl.when(idx >= 12)
        def _():
            swap(q).wait_recv()
            beside(q).wait_recv()
            product(idx, 3, 2.0 * cells,
                    [(stat.at[q], lambda p: own.at[p]), (held.at[q], lambda p: sib.at[p])])

        fold_one(idx).start()

    @pl.when(lead)
    def _():
        columns[g] = jnp.transpose(table[g])
        share().wait_recv()

        @pl.loop(0, len(FOLDED))
        def _(n):
            @pl.when(n < tasks)
            def _():
                step(task_at(n))

            @pl.loop(reached(FOLDED, n - 1), reached(FOLDED, n))
            def _(m):
                absorb_one(task_at(m))

            @pl.loop(reached(SUMMED, n - 1), reached(SUMMED, n))
            def _(m):
                absorb_two(task_at(m))

    @pl.when(aux)
    def _():
        @pl.loop(4, tasks)
        def _(n):
            deliver(task_at(n))

    def store(r, piece):
        down = pl.ds(pl.multiple_of(r * width, width), width)
        along = pl.ds(pl.multiple_of(piece * width, width), width)
        return pltpu.make_async_copy(result.at[r, piece], out_ref.at[down, along], store_done.at[r, piece])

    lanes[...] = jnp.zeros_like(lanes)
    height = 2 * width

    @pl.loop(0, 8)
    def _(n):
        piece = n // 2
        r = n % 2
        mine = (chip == piece) & (crossing | (chip == g) | inner)

        @pl.when(jnp.logical_not(mine & lead))
        def _():
            remote(outn.at[0], inbox.at[side, r, piece], norm_send.at[0], in_recv.at[side, r, piece],
                   (other, g)).wait_recv()

        @pl.when(crossing)
        def _():
            remote(outn.at[0], inbox.at[1 - side, r, piece], norm_send.at[0], in_recv.at[1 - side, r, piece],
                   (other, g)).wait_recv()
        total = inbox[0, r, piece].astype(jnp.int32) + inbox[1, r, piece].astype(jnp.int32)
        result[r, piece] = total.astype(jnp.int16)
        store(r, piece).start()
        value = total.astype(jnp.float32) * (1.0 / UNIT)
        square = value * value
        powered = square * square * square
        rows = c * height + r * width + lax.broadcasted_iota(jnp.int32, (width, width), 0)
        cols = g * block + piece * width + lax.broadcasted_iota(jnp.int32, (width, width), 1)
        powered = jnp.where(rows == cols, 0.0, powered)
        down = pl.ds(pl.multiple_of(r * width, width), width)
        part = powered[:, 0:128]
        for lane in range(1, width // 128):
            part = part + powered[:, lane * 128:(lane + 1) * 128]
        lanes[down, :] = lanes[down, :] + part

    cmsg[...] = jnp.broadcast_to(jnp.sum(jnp.transpose(lanes[...]), axis=0, keepdims=True), cmsg.shape)
    for d in range(1, 4):
        conn_to(d).start()
    for d in range(1, 8):
        local_sums(d).wait_send()
    @pl.when(lead)
    def _():
        genes_to(pair).wait_send()

    @pl.when(aux)
    def _():
        genes_to(beyond).wait_send()
        genes_to(farther).wait_send()

    @pl.when(aux)
    def _():
        share().wait_send()

    @pl.when(aux & inner)
    def _():
        for q in range(4):
            across(q).wait_send()
            relay(q).wait_send()
            beside(q).wait_send()
        for t in range(8):
            passed(t).wait_send()
            onward(t).wait_send()

    @pl.when(lead & outer)
    def _():
        for q in range(4):
            swap(q).wait_send()

    @pl.when(lead)
    def _():
        @pl.loop(0, tasks)
        def _(idx):
            fold_one(idx).wait_send()
            fold_two(idx).wait_send()

            @pl.when(idx >= 4)
            def _():
                hand(idx).wait_send()

            @pl.when(jnp.logical_not(normal_here(idx)))
            def _():
                normal(idx).wait_send()

    @pl.when(aux)
    def _():
        @pl.loop(4, tasks)
        def _(idx):
            turned(idx).wait_send()

    cin[g] = cmsg[...]
    for d in range(1, 4):
        conn_from(d).wait_recv()
    conn_ref[...] = ((cin[0] + cin[1]) + (cin[2] + cin[3]))[0:1]

    @pl.loop(0, 8)
    def _(n):
        store(n % 2, n // 2).wait()
    for d in range(1, 4):
        conn_to(d).wait_send()


def by_planes(counts, library):
    cells, block = counts.shape
    width = block // QUARTERS
    slab = 128
    vmem = pl.BlockSpec(memory_space=pltpu.VMEM)
    anywhere = pl.BlockSpec(memory_space=pl.ANY)
    dma = pltpu.SemaphoreType.DMA
    small = jnp.int16
    count = 16
    quarters = pltpu.VMEM((QUARTERS, width, cells), jnp.bfloat16)
    pieces = pltpu.VMEM((count, width, width), small)
    row = pltpu.VMEM((8, block), jnp.float32)
    totals, connectivity = pl.pallas_call(
        planes,
        out_shape=(
            jax.ShapeDtypeStruct((2 * width, block), small),
            jax.ShapeDtypeStruct((1, 2 * width), jnp.float32),
        ),
        in_specs=[anywhere, vmem],
        out_specs=(anywhere, vmem),
        scratch_shapes=[
            pltpu.VMEM((cells // slab, slab, block), jnp.int32),
            quarters, row, row,
            pltpu.VMEM((2, 4, width, width), small),
            quarters, quarters, quarters,
            pltpu.VMEM((8, width, cells), jnp.bfloat16),
            pltpu.VMEM((count, 4, width, width), small),
            pltpu.VMEM((count, 2, width, width), small),
            pieces, pieces, pieces, pieces,
            pltpu.VMEM((2, 2, 4, width, width), small),
            pltpu.VMEM((8, 8, block), jnp.float32),
            row,
            pltpu.VMEM((4, 8, block), jnp.float32),
            pltpu.VMEM((4, block, 8), jnp.float32),
            pltpu.VMEM((2 * width, 128), jnp.float32),
            pltpu.VMEM((8, 2 * width), jnp.float32),
            pltpu.VMEM((4, 8, 2 * width), jnp.float32),
            dma((4,)), dma((4,)), dma((4,)), dma((4,)), dma, dma, dma((8,)), dma((8,)), dma((8,)), dma((8,)), pltpu.SemaphoreType.REGULAR,
            dma((count,)), dma((count,)), dma((count,)), dma((count,)), dma((count,)), dma((count,)),
            dma((count,)), dma((count,)), dma((2, 2, 4)),
            dma((cells // slab,)), dma((2, 4)),
            dma((8,)), dma((8,)), dma((4,)), dma((4,)), dma((4,)), dma((4,)),
        ],
        compiler_params=pltpu.CompilerParams(
            collective_id=1, has_side_effects=True, vmem_limit_bytes=58 * 1024 * 1024),
    )(counts, library.reshape(cells // slab, slab))
    value = totals.astype(jnp.float32) * (1.0 / UNIT)
    square = value * value
    rows = lax.axis_index("cells") * 2 * width + jnp.arange(2 * width, dtype=jnp.int32)[:, None]
    cols = lax.axis_index("genes") * block + jnp.arange(block, dtype=jnp.int32)[None, :]
    adjacency = jnp.where(rows == cols, jnp.float32(0.0), square * square * square)
    return adjacency, connectivity.reshape(2 * width)


def network(cell_groups, gene_groups, xq_ref, own_ref, sums_ref, out_ref, stats_ref,
            held, partial, landed, totals, sums_in,
            ring_send, ring_recv, cut_send, cut_recv, fly_send, fly_recv, stat_send, stat_recv):
    owners, chunks, part, cells = xq_ref.shape
    rows = owners * part
    cols = own_ref.shape[1]
    half = cols // 2
    c = lax.axis_index("cells")
    g = lax.axis_index("genes")
    right = lax.rem(g + 1, gene_groups)
    left = lax.rem(g + gene_groups - 1, gene_groups)
    bits = cell_groups.bit_length() - 1
    hops = gene_groups - 1
    orders = (tuple(range(bits)), (0,) + tuple(range(bits - 1, 0, -1)))

    barrier = pltpu.get_barrier_semaphore()
    for target in [(c, left), (c, right)] + [(flip(c, b), g) for b in range(bits)]:
        pl.semaphore_signal(barrier, inc=1, device_id=target, device_id_type=pl.DeviceIdType.MESH)
    pl.semaphore_wait(barrier, 2 + bits)

    def ring(q, hop, piece):
        span = pl.ds(piece * (owners // 2), owners // 2)
        source = xq_ref.at[span, q] if hop == 0 else held.at[q, hop - 1, span]
        return pltpu.make_async_remote_copy(
            src_ref=source, dst_ref=held.at[q, hop, span],
            send_sem=ring_send.at[q, hop, piece], recv_sem=ring_recv.at[q, hop, piece],
            device_id=(c, right), device_id_type=pl.DeviceIdType.MESH)

    def cut(q, side, stage):
        count = cell_groups >> (stage + 1)
        return pltpu.make_async_remote_copy(
            src_ref=partial.at[q, side, pl.ds(count, count)],
            dst_ref=landed.at[q, side, pl.ds(count, count)],
            send_sem=cut_send.at[q, side, stage], recv_sem=cut_recv.at[q, side, stage],
            device_id=(flip(c, orders[side][stage]), g), device_id_type=pl.DeviceIdType.MESH)

    def fly(stage):
        return pltpu.make_async_remote_copy(
            src_ref=totals.at[stage], dst_ref=sums_in.at[stage],
            send_sem=fly_send.at[stage], recv_sem=fly_recv.at[stage],
            device_id=(flip(c, stage), g), device_id_type=pl.DeviceIdType.MESH)

    def spread(hop):
        source = totals.at[bits] if hop == 0 else stats_ref.at[hop]
        return pltpu.make_async_remote_copy(
            src_ref=source, dst_ref=stats_ref.at[hop + 1],
            send_sem=stat_send.at[hop], recv_sem=stat_recv.at[hop],
            device_id=(c, right), device_id_type=pl.DeviceIdType.MESH)

    def place(owner, side):
        total = 0
        for position, b in enumerate(orders[side]):
            total = total + ((bit(owner, b) + bit(c, b)) % 2) * (1 << (bits - 1 - position))
        return total

    def multiply(q, step):
        source = lax.rem(g - step + gene_groups, gene_groups)
        block = xq_ref.at[:, q] if step == 0 else held.at[q, step - 1]
        for side in range(2):
            spots = [place(source * owners + o, side) for o in range(owners)]

            @pl.loop(0, half // TILE)
            def _(t):
                start = pl.multiple_of(t * TILE, TILE)
                columns = pl.ds(pl.multiple_of(side * half + start, TILE), TILE)
                tile = jnp.dot(block[...].reshape(rows, cells), own_ref[:, columns], preferred_element_type=jnp.float32)
                for o in range(owners):
                    partial[q, side, spots[o], :, pl.ds(start, TILE)] = tile[o * part:(o + 1) * part]

    def launch(q, stage):
        for side in range(2):
            cut(q, side, stage).start()

    def absorb(q, stage):
        count = cell_groups >> (stage + 1)
        for side in range(2):
            cut(q, side, stage).wait_recv()
            if count > 1:
                @pl.loop(0, count)
                def _(i):
                    partial[q, side, i] = partial[q, side, i] + landed[q, side, i + count]
            else:
                out_ref[pl.ds(q * part, part), side * half:(side + 1) * half] = (
                    partial[q, side, 0] + landed[q, side, 1])

    for piece in range(2):
        ring(0, 0, piece).start()
    totals[0] = sums_ref[...]
    for stage in range(bits):
        fly(stage).start()
        fly(stage).wait_recv()
        totals[stage + 1] = totals[stage] + sums_in[stage]
    stats_ref[0] = totals[bits]

    turns = [[s for s in range(bits) if s * hops // bits == h] for h in range(hops)]

    @pl.loop(0, chunks)
    def _(q):
        multiply(q, 0)
        for hop in range(hops):
            for piece in range(2):
                ring(q, hop, piece).wait_recv()
                if hop < hops - 1:
                    ring(q, hop + 1, piece).start()
            if hop == max(hops - 2, 0):
                @pl.when(q < chunks - 1)
                def _():
                    for piece in range(2):
                        ring(q + 1, 0, piece).start()

            @pl.when(q > 0)
            def _():
                for stage in turns[hop]:
                    absorb(q - 1, stage)
                    if stage + 1 < bits:
                        launch(q - 1, stage + 1)
            multiply(q, hop + 1)
        launch(q, 0)

    last = chunks - 1
    spread(0).start()
    for stage in range(bits):
        absorb(last, stage)
        if stage + 1 < bits:
            launch(last, stage + 1)
        if stage < hops:
            spread(stage).wait_recv()
            if stage + 1 < hops:
                spread(stage + 1).start()
    for hop in range(bits, hops):
        spread(hop).wait_recv()
        if hop + 1 < hops:
            spread(hop + 1).start()
    for hop in range(hops):
        spread(hop).wait_send()
    for stage in range(bits):
        fly(stage).wait_send()

    @pl.loop(0, chunks)
    def _(q):
        for hop in range(hops):
            for piece in range(2):
                ring(q, hop, piece).wait_send()
        for side in range(2):
            for stage in range(bits):
                cut(q, side, stage).wait_send()


def normalize(counts, library):
    factor = 10000.0 / library.astype(jnp.float32)
    return jnp.log1p(counts.astype(jnp.float32) * factor[:, None]).astype(jnp.bfloat16)


def shards(counts, library):
    own_block = normalize(counts, library)
    cells, col_width = own_block.shape
    cell_groups = lax.axis_size("cells")
    gene_groups = lax.axis_size("genes")
    row_width = col_width * gene_groups // cell_groups
    owners = col_width // row_width
    total_cells = float(cells * cell_groups)
    me = lax.axis_index("genes")

    chunks = min(CHUNKS, row_width // 16)
    part = row_width // chunks
    ordered = own_block.T.reshape(owners, chunks, part, cells)
    widened = own_block.astype(jnp.float32)
    sums = jnp.stack([jnp.sum(widened, axis=0), jnp.sum(widened * widened, axis=0)])
    sums = jnp.concatenate([sums, jnp.zeros((6, col_width), jnp.float32)], axis=0)
    bits = cell_groups.bit_length() - 1
    hops = gene_groups - 1
    vmem = pl.BlockSpec(memory_space=pltpu.VMEM)
    dma = pltpu.SemaphoreType.DMA
    gram_tile, stats = pl.pallas_call(
        functools.partial(network, cell_groups, gene_groups),
        out_shape=(
            jax.ShapeDtypeStruct((row_width, col_width), jnp.float32),
            jax.ShapeDtypeStruct((gene_groups, 8, col_width), jnp.float32),
        ),
        in_specs=[vmem] * 3,
        out_specs=(vmem, vmem),
        scratch_shapes=[
            pltpu.VMEM((chunks, hops, owners, part, cells), jnp.bfloat16),
            pltpu.VMEM((chunks, 2, cell_groups, part, col_width // 2), jnp.float32),
            pltpu.VMEM((chunks, 2, cell_groups, part, col_width // 2), jnp.float32),
            pltpu.VMEM((bits + 1, 8, col_width), jnp.float32),
            pltpu.VMEM((bits, 8, col_width), jnp.float32),
            dma((chunks, hops, 2)), dma((chunks, hops, 2)),
            dma((chunks, 2, bits)), dma((chunks, 2, bits)),
            dma((bits,)), dma((bits,)),
            dma((hops,)), dma((hops,)),
        ],
        compiler_params=pltpu.CompilerParams(
            collective_id=0, has_side_effects=True, vmem_limit_bytes=60 * 1024 * 1024),
    )(ordered, own_block, sums)
    order = lax.rem(me - jnp.arange(gene_groups) + gene_groups, gene_groups)
    all_sums = jnp.transpose(jnp.take(stats[:, :2], order, axis=0), (1, 0, 2)).reshape(2, -1)

    means = all_sums[0] / total_cells
    variances = all_sums[1] / total_cells - means * means
    scales = lax.rsqrt(variances + 1e-05)
    row_first = lax.axis_index("cells") * row_width
    col_first = me * col_width
    row_means = lax.dynamic_slice_in_dim(means, row_first, row_width, 0)
    col_means = lax.dynamic_slice_in_dim(means, col_first, col_width, 0)
    row_scales = lax.dynamic_slice_in_dim(scales, row_first, row_width, 0)
    col_scales = lax.dynamic_slice_in_dim(scales, col_first, col_width, 0)
    correlation = (
        (gram_tile / total_cells - row_means[:, None] * col_means[None, :])
        * row_scales[:, None]
        * col_scales[None, :]
    )
    powered = correlation**6
    row_index = row_first + jnp.arange(row_width, dtype=jnp.int32)[:, None]
    col_index = col_first + jnp.arange(col_width, dtype=jnp.int32)[None, :]
    adjacency = jnp.where(row_index == col_index, jnp.float32(0.0), powered)
    connectivity = lax.psum(jnp.sum(adjacency, axis=1), "genes")
    return (adjacency, connectivity)


def solution(mesh):
    sized = mesh.shape["genes"] == 4 and mesh.shape["cells"] == 8

    def body(counts, library):
        cells, block = counts.shape
        if sized and cells % 1024 == 0 and block % 512 == 0:
            return by_planes(counts, library)
        return shards(counts, library)

    return jax.shard_map(
        body,
        mesh=mesh,
        in_specs=(P("cells", "genes"), P("cells")),
        out_specs=(P("cells", "genes"), P("cells")),
        check_vma=False,
    )
```
